512 devices in a mesh: ga: 32 (over y, x, core), ka: 16 (over z).
Axes of the slice: x: 4, y: 4, z: 16, core: 2. Of those that a mesh axis runs over, the one named last changes fastest.
Arguments:
- fine_waves: bfloat16 [256, 16, 40960], P('ka', None, 'ga'), may hold values from -6 to 6
- coarse_waves: bfloat16 [128, 16, 40960], P('ka', None, 'ga'), may hold values from -6 to 6
- coarse_kernel: bfloat16 [192, 64, 8192], P('ga', None, 'ka'), may hold values from -6 to 6
- row_valence: float32 [32, 8, 8, 8], P('ga'), may hold values from -6 to 6
- row_conduction: float32 [32, 8, 8, 8], P('ga'), may hold values from -6 to 6
- row_neighbours: int32 [32, 8], P('ga'), may hold values from 0 to 11, as said below
- row_weight_index: int32 [32, 8], P('ga'), may hold values from 0 to 7
- col_neighbours: int32 [256, 8], P('ka'), may hold values from 0 to 31, as said below
- col_weight_index: int32 [256, 8], P('ka'), may hold values from 0 to 7
- tile_list: int32 [16, 32], replicated, may hold values from 0 to 127, as said below
- weight_table: float32 [8], replicated, may hold values from 0.2 to 0.5
Outputs:
- fine_kernel: bfloat16 [32, 256, 4096], P('ga', 'ka')
The draws below stay inside these ranges and needn't reach their ends.
Inputs may be any that keep to these rules, and one draw needn't show every extreme that they name: `row_neighbours`: each row names 8 distinct positions; a position p below 6 is coarse row p of the fine row's own group r, a larger one is coarse row p - 6 of the next group (the last group's next is group 0); each row names three or more of each kind. `col_neighbours`: each fine column names 8 distinct positions of its owner's list, and every position of the list is named by some column of that owner. `tile_list`: row o lists 32 distinct coarse columns in rising order of their holder (column p is held by owner p // 8); no row takes more than 4 columns from one holder, and every row takes exactly 4 from some holder.
All inputs are finite; a program needn't handle non-finite values.
Results may differ from the reference program's by a relative error of at most 0.0064.
Values may be sent and summed in bfloat16 or wider, within the bound.
A program may use at most 64 MiB of HBM per device.

```python
import math
import jax
import jax.numpy as jnp
from jax import lax

VALENCE = 8
CONDUCTION = 8
PLANE_WAVES = 40960
CORNERS = 8
BAND_PAIRS = 64
ROWS_DEVICE = 1
SLAB_ROWS = 32
GROUP_ROWS = 6
COARSE_ROWS = 192
OWNER_COLUMNS = 16
FINE_COLUMNS = 256
OWNER_COARSE = 8
COARSE_COLUMNS = 128
SLOT_COUNT = 4
LIST_LENGTH = 32
WEIGHT_LEVELS = 8
N_KA = 16


def draw_row_neighbours(key, part):
    row_keys = jax.random.split(key, SLAB_ROWS)

    def one_row(subkey):
        first_key, second_key, third_key = jax.random.split(subkey, 3)
        own_rows = jax.random.permutation(first_key, GROUP_ROWS)
        next_rows = jax.random.permutation(second_key, GROUP_ROWS) + GROUP_ROWS
        remaining = jnp.concatenate([own_rows[3:], next_rows[3:]])
        extra_rows = jax.random.permutation(third_key, remaining)[:2]
        return jnp.concatenate([own_rows[:3], next_rows[:3], extra_rows]).astype(jnp.int32)
    return jax.vmap(one_row)(row_keys)


def draw_col_neighbours(key, part):
    owner_key, column_key = jax.random.split(key)
    owner_keys = jax.random.split(owner_key, N_KA)
    covering = jax.vmap(lambda subkey: jax.random.permutation(subkey, LIST_LENGTH).reshape(LIST_LENGTH // CORNERS, CORNERS))(owner_keys)
    column_keys = jax.random.split(column_key, FINE_COLUMNS)
    picked = jax.vmap(lambda subkey: jax.random.permutation(subkey, LIST_LENGTH)[:CORNERS])(column_keys)
    picked = picked.reshape(N_KA, OWNER_COLUMNS, CORNERS)
    merged = picked.at[:, :LIST_LENGTH // CORNERS].set(covering)
    return merged.reshape(FINE_COLUMNS, CORNERS).astype(jnp.int32)


def draw_tile_list(key, part):
    owner_keys = jax.random.split(key, N_KA)

    def one_list(subkey):
        order_key, column_key = jax.random.split(subkey)
        holder_order = jax.random.permutation(order_key, N_KA)
        standing = jnp.zeros((N_KA,), jnp.int32).at[holder_order].set(jnp.arange(N_KA, dtype=jnp.int32))
        counts = jnp.where(standing < N_KA // 4, SLOT_COUNT, jnp.where(standing < N_KA // 2, 0, SLOT_COUNT // 2))
        column_keys = jax.random.split(column_key, N_KA)
        picked = jax.vmap(lambda inner: jax.random.permutation(inner, OWNER_COARSE)[:SLOT_COUNT])(column_keys)
        column_ids = picked + jnp.arange(N_KA, dtype=jnp.int32)[:, None] * OWNER_COARSE
        filled = jnp.arange(SLOT_COUNT, dtype=jnp.int32)[None, :] < counts[:, None]
        keep_order = jnp.argsort(jnp.where(filled, 0, 1).reshape(-1), stable=True)[:LIST_LENGTH]
        return column_ids.reshape(-1)[keep_order]
    return jax.vmap(one_list)(owner_keys).astype(jnp.int32)


def touch_ends(values, stream_key, least, top_value):
    spot = [jax.random.randint(jax.random.fold_in(stream_key, axis), (), 0, length) for axis, length in enumerate(values.shape)]
    main_axis = values.shape.index(max(values.shape))
    beside = spot[:main_axis] + [(spot[main_axis] + 1) % values.shape[main_axis]] + spot[main_axis + 1:]
    return values.at[tuple(spot)].set(least).at[tuple(beside)].set(top_value)


def level_of(stream_key, dims, shards, least, top_value):
    gain, own = 1.0, jax.random.fold_in(stream_key, 6)
    for dim, parts in shards:
        draws = jnp.exp(jax.random.uniform(jax.random.fold_in(own, dim), (parts,), jnp.float32, least / len(shards), top_value / len(shards)))
        gain = gain * jnp.repeat(draws, dims[dim] // parts).reshape([-1 if axis == dim else 1 for axis in range(len(dims))])
    return gain


def gaussian(own_key, shape, scale, bound, shards=(), kind=jnp.bfloat16):
    values = jax.random.normal(own_key, shape, jnp.float32) * scale
    if len(shards) > 0:
        values = level_of(own_key, shape, shards, -0.22, 0.18) * values
    return jnp.clip(values, min=-bound, max=bound).astype(kind)


def setup_inputs(seed: int = 0) -> dict:
    streams_of = jax.random.split(jax.random.key(seed), 12)
    return {
        "fine_waves": gaussian(streams_of[0], (FINE_COLUMNS, VALENCE + CONDUCTION, PLANE_WAVES), 1.0, 6.0, ((0, 16), (2, 32))),
        "coarse_waves": gaussian(streams_of[1], (COARSE_COLUMNS, VALENCE + CONDUCTION, PLANE_WAVES), 1.0, 6.0, ((0, 16), (2, 32))),
        "coarse_kernel": gaussian(streams_of[2], (COARSE_ROWS, BAND_PAIRS, COARSE_COLUMNS * BAND_PAIRS), 1.0, 6.0, ((0, 32), (2, 16))),
        "row_valence": gaussian(streams_of[3], (SLAB_ROWS, CORNERS, VALENCE, VALENCE), 1.0, 6.0, ((0, 32),), jnp.float32),
        "row_conduction": gaussian(streams_of[4], (SLAB_ROWS, CORNERS, CONDUCTION, CONDUCTION), 1.0, 6.0, ((0, 32),), jnp.float32),
        "row_neighbours": draw_row_neighbours(jax.random.fold_in(streams_of[11], 71), 0),
        "row_weight_index": touch_ends(jax.random.randint(streams_of[6], (SLAB_ROWS, CORNERS), 0, WEIGHT_LEVELS), jax.random.fold_in(streams_of[6], 1), 0, WEIGHT_LEVELS - 1).astype(jnp.int32),
        "col_neighbours": draw_col_neighbours(jax.random.fold_in(streams_of[11], 71), 0),
        "col_weight_index": touch_ends(jax.random.randint(streams_of[8], (FINE_COLUMNS, CORNERS), 0, WEIGHT_LEVELS), jax.random.fold_in(streams_of[8], 1), 0, WEIGHT_LEVELS - 1).astype(jnp.int32),
        "tile_list": draw_tile_list(jax.random.fold_in(streams_of[11], 71), 0),
        "weight_table": jnp.clip(jax.random.uniform(streams_of[10], (WEIGHT_LEVELS,), jnp.float32, 0.2, 0.5), 0.2, 0.5),
    }


def table_lookup(indices, weight_table):
    levels = jnp.arange(weight_table.shape[0], dtype=jnp.int32)
    return lax.optimization_barrier(jnp.sum(jnp.where(indices[..., None] == levels, weight_table, 0.0), axis=-1))

def rotation(weights, valence_part, conduction_part):
    outer_product = jnp.einsum('...vw,...xy->...vxwy', valence_part, conduction_part)
    tile_shape = outer_product.shape[:-4] + (BAND_PAIRS, BAND_PAIRS)
    scaled = weights[..., None, None] * outer_product.reshape(tile_shape) / math.sqrt(BAND_PAIRS)
    return scaled.astype(jnp.bfloat16)

def reference(fine_waves, coarse_waves, coarse_kernel, row_valence, row_conduction, row_neighbours, row_weight_index, col_neighbours, col_weight_index, tile_list, weight_table):
    inv_root = 1.0 / math.sqrt(PLANE_WAVES)
    row_rotation = rotation(table_lookup(row_weight_index, weight_table), row_valence, row_conduction)
    groups = jnp.arange(SLAB_ROWS, dtype=jnp.int32) // ROWS_DEVICE
    row_coarse = ((groups[:, None] * GROUP_ROWS + row_neighbours) % COARSE_ROWS).astype(jnp.int32)
    row_mats = jnp.transpose(row_rotation, (0, 2, 1, 3)).reshape(SLAB_ROWS, BAND_PAIRS, CORNERS * BAND_PAIRS)
    kernel_tiles = coarse_kernel.reshape(COARSE_ROWS, BAND_PAIRS, COARSE_COLUMNS, BAND_PAIRS)

    def per_owner(owner_index):
        listed = tile_list[owner_index]
        start = (owner_index * OWNER_COLUMNS).astype(jnp.int32)
        fine_block = lax.dynamic_slice_in_dim(fine_waves, start, OWNER_COLUMNS, 0).astype(jnp.float32)
        neighbours = lax.dynamic_slice_in_dim(col_neighbours, start, OWNER_COLUMNS, 0)
        weight_levels = lax.dynamic_slice_in_dim(col_weight_index, start, OWNER_COLUMNS, 0)
        list_waves = jnp.take(coarse_waves, listed, axis=0)
        valence_terms = []
        conduction_terms = []
        for corner in range(CORNERS):
            paired = jnp.take(list_waves, neighbours[:, corner], axis=0).astype(jnp.float32)
            valence_terms.append(jnp.einsum('fvg,fwg->fvw', fine_block[:, :VALENCE], paired[:, :VALENCE]))
            conduction_terms.append(jnp.einsum('fvg,fwg->fvw', fine_block[:, VALENCE:], paired[:, VALENCE:]))
        valence_correlation = jnp.stack(valence_terms, 1) * inv_root
        conduction_correlation = jnp.stack(conduction_terms, 1) * inv_root
        col_rotation = rotation(table_lookup(weight_levels, weight_table), valence_correlation, conduction_correlation)
        listed_tiles = jnp.take(kernel_tiles, listed, axis=2).reshape(COARSE_ROWS, BAND_PAIRS, LIST_LENGTH * BAND_PAIRS)

        def per_row(row_item):
            rotation_matrix, coarse_rows = row_item
            chosen = jnp.take(listed_tiles, coarse_rows, axis=0).reshape(CORNERS * BAND_PAIRS, LIST_LENGTH * BAND_PAIRS)
            product = jnp.dot(rotation_matrix.astype(jnp.float32), chosen.astype(jnp.float32), preferred_element_type=jnp.float32)
            return product.astype(jnp.bfloat16)
        left_tiles = lax.map(per_row, (row_mats, row_coarse)).reshape(SLAB_ROWS, BAND_PAIRS, LIST_LENGTH, BAND_PAIRS)
        gathered = jnp.take(left_tiles, neighbours, axis=2)
        result = jnp.einsum('rafjb,fjcb->rfac', gathered.astype(jnp.float32), col_rotation.astype(jnp.float32))
        return result.reshape(SLAB_ROWS, OWNER_COLUMNS, BAND_PAIRS * BAND_PAIRS).astype(jnp.bfloat16)
    blocks = lax.map(per_owner, jnp.arange(N_KA, dtype=jnp.int32))
    return jnp.transpose(blocks, (1, 0, 2, 3)).reshape(SLAB_ROWS, FINE_COLUMNS, BAND_PAIRS * BAND_PAIRS)
```

```python
import functools
import math

import jax
import jax.numpy as jnp
from jax import lax
from jax.experimental import pallas as pl
from jax.experimental.pallas import tpu as pltpu
from jax.sharding import PartitionSpec as P

MESH = pl.DeviceIdType.MESH
PLANE_WAVES = 40960
CORNERS = 8
PAIRS = 64
BANDS = 16
F32 = jnp.float32
BF16 = jnp.bfloat16
LAG = 2


def lanes(shape):
    return lax.broadcasted_iota(jnp.int32, shape, len(shape) - 1)


def kernel(
    nz, row_peers, line_peers,
    fine_hbm, coarse_hbm, tiles_hbm, rv, rc, rn, rwi, cn, cwi, tl, wt,
    out,
    fine, waves, dense, stack, left, spread, expanded, rsm, mixed, sel, from_row, sum1,
    from_line, sum2, full, off_d, off_l, wgt,
    in_sem, ws, wr, up_s, up_r, ts, tr, rs_s, rs_r, ln_s, ln_r, ag_s, ag_r,
):
    g, z = lax.axis_index("ga"), lax.axis_index("ka")
    ng = row_peers * line_peers
    half = nz // 2
    col_rows = waves.shape[1] // 2
    y, j_me = g // row_peers, lax.rem(g, row_peers)
    nbr = (lax.rem(z + 1, nz), lax.rem(z + nz - 1, nz))

    get_coarse = pltpu.make_async_copy(coarse_hbm, waves.at[0], in_sem.at[0])
    get_tiles = pltpu.make_async_copy(tiles_hbm, stack.at[pl.ds(0, 6)], in_sem.at[1])
    get_fine = pltpu.make_async_copy(fine_hbm, fine, in_sem.at[2])
    get_coarse.start()
    get_tiles.start()
    get_fine.start()

    def row_peer(r):
        return y * row_peers + lax.rem(j_me + r, row_peers)

    def line_peer(r):
        return lax.rem(y + r, line_peers) * row_peers + j_me

    up_to, up_from = lax.rem(g + ng - 1, ng), lax.rem(g + 1, ng)
    barrier = pltpu.get_barrier_semaphore()
    friends = [(g, nbr[0]), (g, nbr[1]), (up_to, z), (up_from, z)]
    friends += [(row_peer(r), z) for r in range(1, row_peers)]
    friends += [(line_peer(r), z) for r in range(1, line_peers)]
    for who in friends:
        pl.semaphore_signal(barrier, inc=1, device_id=who, device_id_type=MESH)
    pl.semaphore_wait(barrier, len(friends))

    def slot(way, d):
        return lax.rem(nz - d, nz) if way == 0 else d

    def wave(way, d, j):
        rows = pl.ds(j * col_rows, col_rows)
        return pltpu.make_async_remote_copy(
            src_ref=waves.at[slot(way, d - 1), rows],
            dst_ref=waves.at[slot(way, d), rows],
            send_sem=ws.at[way, d - 1, j],
            recv_sem=wr.at[way, d - 1, j],
            device_id=(g, nbr[way]),
            device_id_type=MESH,
        )

    def tile(way, k, part=None):
        first, count = (0, 4) if part is None else (part * 2, 2)
        return pltpu.make_async_remote_copy(
            src_ref=left.at[pl.ds(slot(way, k - 1) * 4 + first, count)],
            dst_ref=left.at[pl.ds(slot(way, k) * 4 + first, count)],
            send_sem=ts.at[way, k - 1],
            recv_sem=tr.at[way, k - 1],
            device_id=(g, nbr[way]),
            device_id_type=MESH,
        )

    def swap(base, count):
        for q in range(count):
            v = left[base + q].astype(F32)
            left[nz * 4 + base + q] = pltpu.roll(v, 64, 1).astype(BF16)

    def correlate(s, j):
        part = waves[s, pl.ds(j * col_rows, col_rows), :]
        at = (s * (2 * col_rows) + j * col_rows) // 8
        both = lax.dot_general(
            part, fine[...], (((1,), (1,)), ((), ())), preferred_element_type=F32
        )
        dense[pl.ds(at, col_rows // 8)] = both.reshape(col_rows // 8, 8, 256)

    get_coarse.wait()
    for jj in range(2):
        wave(0, 1, jj).start()
        wave(1, 1, 1 - jj).start()
    get_tiles.wait()
    upper = pltpu.make_async_remote_copy(
        src_ref=stack.at[pl.ds(0, 6)],
        dst_ref=stack.at[pl.ds(6, 6)],
        send_sem=up_s,
        recv_sem=up_r,
        device_id=(up_to, z),
        device_id_type=MESH,
    )
    upper.start()
    get_fine.wait()
    for j in range(2):
        correlate(0, j)

    scale = 1.0 / (PLANE_WAVES * math.sqrt(PAIRS))

    def place(i, carry):
        f, c = i // CORNERS, i % CORNERS
        col = tl[z, cn[f, c]]
        s = (lax.shift_right_logical(col, 3) - z + nz) & (nz - 1)
        jj = col & 7
        off_d[i] = (s * 8 + jj) * 2
        off_l[i] = s * 4 + lax.shift_right_logical(jj, 1) + ((jj + c) & 1) * (nz * 4)
        wgt[i] = wt[cwi[f, c]] * scale
        return carry

    lax.fori_loop(0, 128, place, 0)

    into = lanes((128, 1024))
    row = lax.broadcasted_iota(jnp.int32, (128, 1024), 0)
    local = into % 512
    wanted = (local // 64) * 16 + jnp.where(into < 512, (local % 64) // 8, 8 + local % 8)
    spread[...] = jnp.where(row == wanted, 1.0, 0.0).astype(BF16)

    def wave_step(d):
        for jj in range(2):
            for way in range(2):
                j = jj if way == 0 else 1 - jj
                wave(way, d, j).wait_recv()
                if jj == 0:
                    wave(way, d + 1, j).start()
                else:

                    @pl.when(d < half - 1)
                    def _():
                        wave(way, d + 1, j).start()

                correlate(slot(way, d), j)

    wave_step(1)

    wide = lanes((8, PAIRS))
    low = lax.broadcasted_iota(jnp.int32, (8, PAIRS), 0)
    to_w = jnp.where(wide // 8 == low, 1.0, 0.0)
    to_y = jnp.where(wide % 8 == low, 1.0, 0.0)
    exact = lax.Precision.HIGHEST
    row_v = jnp.dot(rv[...], to_w, precision=exact, preferred_element_type=F32)
    row_c = jnp.dot(rc[...], to_y, precision=exact, preferred_element_type=F32)
    upper.wait_recv()
    rotated = jnp.zeros((PAIRS, stack.shape[2]), F32)
    for c in range(CORNERS):
        w = wt[rwi[0, c]]
        cond = row_c[c * 8 : c * 8 + 8]
        mat = jnp.concatenate(
            [row_v[c * 8 + v : c * 8 + v + 1] * cond for v in range(8)], axis=0
        )
        mat = (w * mat * (1.0 / math.sqrt(PAIRS))).astype(BF16)
        rotated += jnp.dot(mat, stack[rn[0, c]], preferred_element_type=F32)
    rotated = rotated.astype(BF16)
    for q in range(4):
        left[q] = rotated[:, q * 128 : (q + 1) * 128]
    swap(0, 4)

    def tile_step(k, parts=False):
        for way in range(2):
            tile(way, k).wait_recv()
        for way in range(2):
            tile(way, k + 1, way if parts else None).start()
        for way in range(2):
            swap(slot(way, k) * 4, 4)

    def both(d, carry):
        wave_step(d)

        @pl.when(d == 1 + LAG)
        def _():
            for way in range(2):
                tile(way, 1).start()

        @pl.when(d > 1 + LAG)
        def _():
            tile_step(d - 1 - LAG)

        return carry

    lax.fori_loop(2, half, both, 0)
    for way in range(2):
        wave(way, half, way).wait_recv()
        correlate(half, way)

    lane = lanes((8, 128))

    def pick(c, carry):
        for t in range(2):
            acc = jnp.zeros((8, 128), F32)
            for ff in range(8):
                i = (t * 8 + ff) * CORNERS + c
                val = dense[off_d[i], :, t * 128 : t * 128 + 128] * wgt[i]
                cond = dense[off_d[i] + 1, :, t * 128 : t * 128 + 128]
                acc = jnp.where(lane // 8 == 2 * ff, val, acc)
                acc = jnp.where(lane // 8 == 2 * ff + 1, cond, acc)
            sel[c, :, pl.ds(t * 128, 128)] = acc
        return carry

    lax.fori_loop(0, CORNERS, pick, 0)

    def to_row(r):
        return pltpu.make_async_remote_copy(
            src_ref=sel.at[lax.rem(j_me + r, row_peers)],
            dst_ref=from_row.at[r - 1],
            send_sem=rs_s.at[r - 1],
            recv_sem=rs_r.at[r - 1],
            device_id=(row_peer(r), z),
            device_id_type=MESH,
        )

    def to_line(r):
        return pltpu.make_async_remote_copy(
            src_ref=sum1,
            dst_ref=from_line.at[r - 1],
            send_sem=ln_s.at[r - 1],
            recv_sem=ln_r.at[r - 1],
            device_id=(line_peer(r), z),
            device_id_type=MESH,
        )

    def to_all(r):
        return pltpu.make_async_remote_copy(
            src_ref=sum2,
            dst_ref=full.at[j_me],
            send_sem=ag_s.at[r - 1],
            recv_sem=ag_r.at[r - 1],
            device_id=(row_peer(r), z),
            device_id_type=MESH,
        )

    def got_all(r):
        return pltpu.make_async_remote_copy(
            src_ref=sum2,
            dst_ref=full.at[lax.rem(j_me + row_peers - r, row_peers)],
            send_sem=ag_s.at[r - 1],
            recv_sem=ag_r.at[r - 1],
            device_id=(row_peer(r), z),
            device_id_type=MESH,
        )

    for r in range(1, row_peers):
        to_row(r).start()
    first_late = half - 1 - LAG
    tile_step(first_late)
    total = sel[j_me]
    for r in range(1, row_peers):
        to_row(r).wait_recv()
        total += from_row[r - 1]
    sum1[...] = total
    for r in range(1, line_peers):
        to_line(r).start()
    tile_step(first_late + 1)
    for r in range(1, line_peers):
        to_line(r).wait_recv()
        total += from_line[r - 1]
    sum2[...] = total
    full[j_me] = total
    for r in range(1, row_peers):
        to_all(r).start()
    tile_step(first_late + 2, parts=True)
    for r in range(1, row_peers):
        got_all(r).wait_recv()

    corr = full[...].reshape(CORNERS * 8, 256)
    corr = jnp.concatenate([corr[:, :128], corr[:, 128:]], axis=0)
    high = corr.astype(BF16)
    rest = (corr - high.astype(F32)).astype(BF16)
    expanded[...] = jnp.dot(high, spread[...], preferred_element_type=F32) + jnp.dot(
        rest, spread[...], preferred_element_type=F32
    )

    def rotate(c, carry):
        for t in range(2):
            at = pl.multiple_of(t * 64 + c * 8, 8)
            val = expanded[pl.ds(at, 8), pl.ds(0, 512)]
            cond = expanded[pl.ds(at, 8), pl.ds(512, 512)]
            for w in range(0, 8, 2):
                both_w = jnp.concatenate([val[w : w + 1] * cond, val[w + 1 : w + 2] * cond], 0)
                to = pl.multiple_of(c * 64 + w * 8, 16)
                rsm[pl.ds(to, 16), pl.ds(t * 512, 512)] = both_w.astype(BF16)
        return carry

    lax.fori_loop(0, CORNERS, rotate, 0)

    for way in range(2):
        tile(way, half, way).wait_recv()
    swap(half * 4, 4)

    near = lanes((64, 128)) < 64

    for p in range(8):
        blocks = []
        for ff in range(2):
            f = p * 2 + ff
            quads = []
            for q in range(4):
                a = left[off_l[f * CORNERS + 2 * q]]
                b = left[off_l[f * CORNERS + 2 * q + 1]]
                quads.append(jnp.where(near, a, b))
            blocks.append(jnp.concatenate(quads, axis=1))
        res = jnp.dot(
            jnp.concatenate(blocks, axis=0),
            rsm[:, p * 128 : (p + 1) * 128],
            preferred_element_type=F32,
        )
        turned = pltpu.roll(res, 64, 1)
        mixed[p * 128 : p * 128 + 64, :] = jnp.where(near, res[:64], turned[:64])
        mixed[p * 128 + 64 : p * 128 + 128, :] = jnp.where(near, turned[64:], res[64:])

    near_f = lanes((16, 128)) < 64
    for t in range(32):
        even = mixed[pl.ds(2 * t, 16, stride=64), :]
        odd = mixed[pl.ds(2 * t + 1, 16, stride=64), :]
        out[:, t * 128 : (t + 1) * 128] = jnp.where(near_f, even, odd).astype(BF16)

    upper.wait_send()

    def sent(d, carry):
        for way in range(2):
            for j in range(2):
                wave(way, d, j).wait_send()
            tile(way, d).wait_send()
        return carry

    lax.fori_loop(1, half, sent, 0)
    for way in range(2):
        wave(way, half, way).wait_send()
        tile(way, half, way).wait_send()
    for r in range(1, row_peers):
        to_row(r).wait_send()
        to_all(r).wait_send()
    for r in range(1, line_peers):
        to_line(r).wait_send()


def body(mesh_shape, *args):
    (fine_waves, coarse_waves, coarse_kernel, row_valence, row_conduction, row_neighbours,
     row_weight_index, col_neighbours, col_weight_index, tile_list, weight_table) = args
    nz, ng = mesh_shape
    row_peers, line_peers = CORNERS, ng // CORNERS
    width = fine_waves.shape[2]
    held = coarse_waves.shape[0] * BANDS
    any_space = pl.BlockSpec(memory_space=pl.ANY)
    vmem = pl.BlockSpec(memory_space=pltpu.VMEM)
    smem = pl.BlockSpec(memory_space=pltpu.SMEM)
    half = nz // 2
    dma = pltpu.SemaphoreType.DMA
    out = pl.pallas_call(
        functools.partial(kernel, nz, row_peers, line_peers),
        out_shape=jax.ShapeDtypeStruct((16, PAIRS * PAIRS), BF16),
        in_specs=[any_space] * 3 + [vmem] * 2 + [smem] * 6,
        out_specs=vmem,
        scratch_shapes=[
            pltpu.VMEM((256, width), BF16),
            pltpu.VMEM((nz, held, width), BF16),
            pltpu.VMEM((nz * held // 8, 8, 256), F32),
            pltpu.VMEM((12, PAIRS, 512), BF16),
            pltpu.VMEM((2 * nz * 4, PAIRS, 128), BF16),
            pltpu.VMEM((128, 1024), BF16),
            pltpu.VMEM((128, 1024), F32),
            pltpu.VMEM((512, 1024), BF16),
            pltpu.VMEM((1024, 128), F32),
            pltpu.VMEM((CORNERS, 8, 256), F32),
            pltpu.VMEM((row_peers - 1, 8, 256), F32),
            pltpu.VMEM((8, 256), F32),
            pltpu.VMEM((line_peers - 1, 8, 256), F32),
            pltpu.VMEM((8, 256), F32),
            pltpu.VMEM((CORNERS, 8, 256), F32),
            pltpu.SMEM((128,), jnp.int32),
            pltpu.SMEM((128,), jnp.int32),
            pltpu.SMEM((128,), F32),
            dma((3,)),
            dma((2, half, 2)),
            dma((2, half, 2)),
            dma,
            dma,
            dma((2, half)),
            dma((2, half)),
            dma((row_peers - 1,)),
            dma((row_peers - 1,)),
            dma((line_peers - 1,)),
            dma((line_peers - 1,)),
            dma((row_peers - 1,)),
            dma((row_peers - 1,)),
        ],
        compiler_params=pltpu.CompilerParams(
            collective_id=0, has_side_effects=True, vmem_limit_bytes=40 * 1024 * 1024
        ),
        name="interpolate",
    )(
        fine_waves.reshape(16 * BANDS, width),
        coarse_waves.reshape(held, width),
        coarse_kernel,
        row_valence.reshape(64, 8),
        row_conduction.reshape(64, 8),
        row_neighbours,
        row_weight_index,
        col_neighbours,
        col_weight_index,
        tile_list,
        weight_table,
    )
    return out[None]


def solution(mesh):
    placed = (
        P("ka", None, "ga"),
        P("ka", None, "ga"),
        P("ga", None, "ka"),
        P("ga", None, None, None),
        P("ga", None, None, None),
        P("ga", None),
        P("ga", None),
        P("ka", None),
        P("ka", None),
        P(),
        P(),
    )
    shape = (mesh.shape["ka"], mesh.shape["ga"])
    return jax.shard_map(
        functools.partial(body, shape),
        mesh=mesh,
        in_specs=placed,
        out_specs=P("ga", "ka", None),
        check_vma=False,
    )
```

```python
import functools
import math

import jax
import jax.numpy as jnp
from jax import lax
from jax.experimental import pallas as pl
from jax.experimental.pallas import tpu as pltpu
from jax.sharding import PartitionSpec as P

MESH = pl.DeviceIdType.MESH
PLANE_WAVES = 40960
CORNERS = 8
PAIRS = 64
BANDS = 16
F32 = jnp.float32
BF16 = jnp.bfloat16
NC = 2
NEAR = 5
SLOTS = 4


def lanes(shape):
    return lax.broadcasted_iota(jnp.int32, shape, len(shape) - 1)


def kernel(
    nz, nx, ny,
    fine_hbm, coarse_hbm, tiles_hbm, rv, rc, rn, rwi, cn, cwi, tl, wt,
    out,
    fine, waves, far_w, dense, stack, left, near_t, spread, expanded, rsm, mixed, picked_w, picked_t, sel, from_core,
    part, from_x, sum1, from_y, full, off_d, off_l, wgt, rank, first,
    in_sem, ws, wr, up_s, up_r, ts, tr, far_s, far_r, core_s, core_r, x_s, x_r, y_s, y_r,
):
    g, z = lax.axis_index("ga"), lax.axis_index("ka")
    ng = 2 * nx * ny
    half = nz // 2
    last = half - 2
    assert NEAR == last - 1
    piece = waves.shape[1] // NC
    core = lax.rem(g, 2)
    y, x = g // (2 * nx), lax.rem(g // 2, nx)
    partner = g + 1 - 2 * core

    def away(way, n):
        return lax.rem(z + (n if way == 0 else nz - n), nz)

    nbr = (away(0, 1), away(1, 1))

    get_coarse = pltpu.make_async_copy(coarse_hbm, waves.at[0], in_sem.at[0])
    get_tiles = pltpu.make_async_copy(tiles_hbm, stack.at[pl.ds(0, 6)], in_sem.at[1])
    get_fine = pltpu.make_async_copy(fine_hbm, fine, in_sem.at[2])
    get_coarse.start()
    get_tiles.start()
    get_fine.start()

    def x_peer(r):
        return y * (2 * nx) + 2 * lax.rem(x + r, nx) + core

    def y_peer(r):
        return lax.rem(y + r, ny) * (2 * nx) + 2 * x + core

    up_to, up_from = lax.rem(g + ng - 1, ng), lax.rem(g + 1, ng)
    barrier = pltpu.get_barrier_semaphore()
    friends = [(g, away(way, n)) for n in range(1, half - NEAR + 1) for way in range(2)]
    friends += [(up_to, z), (up_from, z), (partner, z)]
    friends += [(x_peer(r), z) for r in range(1, nx)]
    friends += [(y_peer(r), z) for r in range(1, ny)]
    for who in friends:
        pl.semaphore_signal(barrier, inc=1, device_id=who, device_id_type=MESH)
    pl.semaphore_wait(barrier, len(friends))

    def slot(way, d):
        return lax.rem(nz - d, nz) if way == 0 else d

    def wave(way, d, j):
        cols = pl.ds(j * piece, piece)
        whole = waves.at[slot(way, d), cols]
        return pltpu.make_async_remote_copy(
            src_ref=waves.at[slot(way, d - 1), cols],
            dst_ref=far_w.at[way, cols] if isinstance(d, int) and d == last else whole,
            send_sem=ws.at[way, d - 1, j],
            recv_sem=wr.at[way, d - 1, j],
            device_id=(g, nbr[way]),
            device_id_type=MESH,
        )

    def chosen_wave(way, onward):
        cols = pl.ds(SLOTS, SLOTS // 2) if onward else pl.ds(0, SLOTS)
        j = 0 if onward else 1
        return pltpu.make_async_remote_copy(
            src_ref=picked_w.at[way, cols],
            dst_ref=waves.at[slot(way, half - 1), cols],
            send_sem=ws.at[way, half - 2, j],
            recv_sem=wr.at[way, half - 2, j],
            device_id=(g, nbr[way]),
            device_id_type=MESH,
        )

    def last_wave(way):
        return pltpu.make_async_remote_copy(
            src_ref=waves.at[slot(way, half - 1), pl.ds(SLOTS, SLOTS // 2)],
            dst_ref=waves.at[half, pl.ds(way * (SLOTS // 2), SLOTS // 2)],
            send_sem=ws.at[way, half - 1, 0],
            recv_sem=wr.at[way, half - 1, 0],
            device_id=(g, nbr[way]),
            device_id_type=MESH,
        )

    def tile(way, k):
        whole = left.at[pl.ds(slot(way, k) * 4, 4)]
        return pltpu.make_async_remote_copy(
            src_ref=left.at[pl.ds(slot(way, k - 1) * 4, 4)],
            dst_ref=near_t.at[way, pl.ds(0, 4)] if isinstance(k, int) and k == NEAR else whole,
            send_sem=ts.at[way, k - 1],
            recv_sem=tr.at[way, k - 1],
            device_id=(g, nbr[way]),
            device_id_type=MESH,
        )

    def far_tile(way, k):
        begin, count = (0, 2) if k < half else (way, 1)
        return pltpu.make_async_remote_copy(
            src_ref=picked_t.at[way, k - NEAR - 1, pl.ds(begin, count)],
            dst_ref=left.at[pl.ds(slot(way, k) * 4 + begin, count)],
            send_sem=far_s.at[way, k - NEAR - 1],
            recv_sem=far_r.at[way, k - NEAR - 1],
            device_id=(g, away(way, k - NEAR)),
            device_id_type=MESH,
        )

    def swap(base, count):
        for q in range(count):
            v = left[base + q].astype(F32)
            left[nz * 4 + base + q] = pltpu.roll(v, 64, 1).astype(BF16)

    def correlate(s, j, way=None):
        block = waves[s, pl.ds(j * 4, 4)] if way is None else far_w[way, pl.ds(j * 4, 4)]
        rows = block.reshape(4 * BANDS, waves.shape[3])
        both = lax.dot_general(
            rows, fine[...], (((1,), (1,)), ((), ())), preferred_element_type=F32
        )
        dense[pl.ds(s * 16 + j * 8, 8)] = both.reshape(8, 8, 256)

    get_coarse.wait()
    for jj in range(NC):
        for way in range(2):
            wave(way, 1, jj).start()
    get_tiles.wait()
    upper = pltpu.make_async_remote_copy(
        src_ref=stack.at[pl.ds(0, 6)],
        dst_ref=stack.at[pl.ds(6, 6)],
        send_sem=up_s,
        recv_sem=up_r,
        device_id=(up_to, z),
        device_id_type=MESH,
    )
    upper.start()
    get_fine.wait()
    for j in range(2):
        correlate(0, j)

    scale = 1.0 / (PLANE_WAVES * math.sqrt(PAIRS))

    def ranks(n, carry):
        before, count = carry
        holder = lax.shift_right_logical(tl[z, n], 3)
        count = jnp.where(holder == before, count + 1, 0)
        rank[n] = count
        return holder, count

    lax.fori_loop(0, tl.shape[1], ranks, (jnp.int32(-1), jnp.int32(0)))

    def place(i, carry):
        f, c = i // CORNERS, i % CORNERS
        n = cn[c, f]
        col = tl[z, n]
        s = (lax.shift_right_logical(col, 3) - z + nz) & (nz - 1)
        hops = jnp.minimum(s, nz - s)
        jj = jnp.where(hops > last, rank[n], col & 7)
        off_d[i] = (s * 8 + jj) * 2
        jj = jnp.where(hops > NEAR, rank[n], col & 7)
        off_l[i] = s * 4 + lax.shift_right_logical(jj, 1) + ((jj + c) & 1) * (nz * 4)
        wgt[i] = wt[cwi[c, f]] * scale
        return carry

    lax.fori_loop(0, 128, place, 0)

    into = lanes((128, 1024))
    row = lax.broadcasted_iota(jnp.int32, (128, 1024), 0)
    local = into % 512
    wanted = (local // 64) * 16 + jnp.where(into < 512, (local % 64) // 8, 8 + local % 8)
    spread[...] = jnp.where(row == wanted, 1.0, 0.0).astype(BF16)

    def wave_step(d):
        for jj in range(NC):
            for way in range(2):
                wave(way, d, jj).wait_recv()
                wave(way, d + 1, jj).start()
            if (jj + 1) * piece % 4 == 0:
                for way in range(2):
                    correlate(slot(way, d), (jj + 1) * piece // 4 - 1)

    wave_step(1)

    wide = lanes((8, PAIRS))
    low = lax.broadcasted_iota(jnp.int32, (8, PAIRS), 0)
    to_w = jnp.where(wide // 8 == low, 1.0, 0.0)
    to_y = jnp.where(wide % 8 == low, 1.0, 0.0)
    exact = lax.Precision.HIGHEST
    row_v = jnp.dot(rv[...], to_w, precision=exact, preferred_element_type=F32)
    row_c = jnp.dot(rc[...], to_y, precision=exact, preferred_element_type=F32)
    upper.wait_recv()
    rotated = jnp.zeros((PAIRS, stack.shape[2]), F32)
    for c in range(CORNERS):
        w = wt[rwi[0, c]]
        cond = row_c[c * 8 : c * 8 + 8]
        mat = jnp.concatenate(
            [row_v[c * 8 + v : c * 8 + v + 1] * cond for v in range(8)], axis=0
        )
        mat = (w * mat * (1.0 / math.sqrt(PAIRS))).astype(BF16)
        rotated += jnp.dot(mat, stack[rn[0, c]], preferred_element_type=F32)
    rotated = rotated.astype(BF16)
    for q in range(4):
        left[q] = rotated[:, q * 128 : (q + 1) * 128]
    swap(0, 4)

    def tile_step(k):
        for way in range(2):
            tile(way, k - 1).wait_recv()
        for way in range(2):
            tile(way, k).start()
        for way in range(2):
            swap(slot(way, k - 1) * 4, 4)

    served = []
    for way in range(2):
        served += [(away(way, n), away(1 - way, last)) for n in (1, 2)]
        served += [(away(way, n), away(1 - way, NEAR)) for n in range(1, half - NEAR + 1)]
    per_way = len(served) // 2

    def starts(n, counts):
        return tuple(
            count + jnp.where(lax.shift_right_logical(tl[o, n], 3) < h, 1, 0)
            for count, (o, h) in zip(counts, served)
        )

    counts = lax.fori_loop(0, tl.shape[1], starts, (jnp.int32(0),) * len(served))
    for i, count in enumerate(counts):
        first[i] = count

    def entry(i, k):
        return tl[served[i][0], jnp.minimum(first[i] + k, tl.shape[1] - 1)] & 7

    for way in range(2):
        tile(way, 1).start()

    def both(d, carry):
        wave_step(d)
        tile_step(d)
        return carry

    lax.fori_loop(2, NEAR, both, 0)
    wave_step(NEAR)
    tile_step(NEAR)
    for way in range(2):
        for jj in range(NC):
            wave(way, last, jj).wait_recv()
    near = lanes((64, 128)) < 64
    for way in range(2):
        for n, (owner, k) in enumerate(
            [(0, k) for k in range(SLOTS)] + [(1, way * 2), (1, way * 2 + 1)]
        ):
            picked_w[way, n] = far_w[way, entry(way * per_way + owner, k)]
    for way in range(2):
        chosen_wave(way, True).start()
    for way in range(2):
        chosen_wave(way, False).start()
    for way in range(2):
        for j in range(2):
            correlate(slot(way, last), j, way)

    for way in range(2):
        tile(way, NEAR).wait_recv()
    for way in range(2):
        s = slot(way, NEAR)
        for q in range(4):
            v = near_t[way, q]
            turned = pltpu.roll(v.astype(F32), 64, 1).astype(BF16)
            near_t[way, 4 + q] = turned
            left[s * 4 + q] = v
            left[nz * 4 + s * 4 + q] = turned
        for n in range(half - NEAR):
            for q in range(2):
                lo = entry(way * per_way + 2 + n, 2 * q)
                hi = entry(way * per_way + 2 + n, 2 * q + 1)
                a = near_t[way, lax.shift_right_logical(lo, 1) + (lo & 1) * 4]
                b = near_t[way, lax.shift_right_logical(hi, 1) + ((hi + 1) & 1) * 4]
                picked_t[way, n, q] = jnp.where(near, a, b)
    for way in range(2):
        chosen_wave(way, True).wait_recv()
        last_wave(way).start()
    for way in range(2):
        chosen_wave(way, False).wait_recv()
        correlate(slot(way, half - 1), 0)
    for way in range(2):
        last_wave(way).wait_recv()
    correlate(half, 0)

    for k in range(half, NEAR, -1):
        for way in range(2):
            far_tile(way, k).start()

    lane = lanes((8, 128))

    def pick(c, carry):
        for t in range(2):
            acc = jnp.zeros((8, 128), F32)
            for ff in range(8):
                i = (t * 8 + ff) * CORNERS + c
                val = dense[off_d[i], :, t * 128 : t * 128 + 128] * wgt[i]
                cond = dense[off_d[i] + 1, :, t * 128 : t * 128 + 128]
                acc = jnp.where(lane // 8 == 2 * ff, val, acc)
                acc = jnp.where(lane // 8 == 2 * ff + 1, cond, acc)
            sel[c, :, pl.ds(t * 128, 128)] = acc
        return carry

    lax.fori_loop(0, CORNERS, pick, 0)

    to_core = pltpu.make_async_remote_copy(
        src_ref=sel.at[pl.ds((1 - core) * nx, nx)],
        dst_ref=from_core,
        send_sem=core_s.at[0],
        recv_sem=core_r.at[0],
        device_id=(partner, z),
        device_id_type=MESH,
    )

    def to_x(r):
        return pltpu.make_async_remote_copy(
            src_ref=part,
            dst_ref=from_x.at[r - 1],
            send_sem=x_s.at[r - 1],
            recv_sem=x_r.at[r - 1],
            device_id=(x_peer(r), z),
            device_id_type=MESH,
        )

    def to_y(r):
        return pltpu.make_async_remote_copy(
            src_ref=sum1,
            dst_ref=from_y.at[r - 1],
            send_sem=y_s.at[r - 1],
            recv_sem=y_r.at[r - 1],
            device_id=(y_peer(r), z),
            device_id_type=MESH,
        )

    def across(arriving=False):
        mine = 1 - core if arriving else core
        return pltpu.make_async_remote_copy(
            src_ref=full.at[pl.ds(core * nx, nx)],
            dst_ref=full.at[pl.ds(mine * nx, nx)],
            send_sem=core_s.at[1],
            recv_sem=core_r.at[1],
            device_id=(partner, z),
            device_id_type=MESH,
        )

    to_core.start()
    to_core.wait_recv()
    total = sel[pl.ds(core * nx, nx)] + from_core[...]
    part[...] = total
    for r in range(1, nx):
        to_x(r).start()
    for r in range(1, nx):
        to_x(r).wait_recv()
        total += from_x[r - 1]
    sum1[...] = total
    for r in range(1, ny):
        to_y(r).start()
    for r in range(1, ny):
        to_y(r).wait_recv()
        total += from_y[r - 1]
    full[pl.ds(core * nx, nx)] = total
    across().start()
    for k in range(NEAR + 1, half):
        for way in range(2):
            far_tile(way, k).wait_recv()
            swap(slot(way, k) * 4, 2)
    for way in range(2):
        far_tile(way, half).wait_recv()
    swap(half * 4, 2)
    across(True).wait_recv()

    corr = full[...].reshape(CORNERS * 8, 256)
    corr = jnp.concatenate([corr[:, :128], corr[:, 128:]], axis=0)
    high = corr.astype(BF16)
    rest = (corr - high.astype(F32)).astype(BF16)
    expanded[...] = jnp.dot(high, spread[...], preferred_element_type=F32) + jnp.dot(
        rest, spread[...], preferred_element_type=F32
    )

    def rotate(c, carry):
        for t in range(2):
            at = pl.multiple_of(t * 64 + c * 8, 8)
            val = expanded[pl.ds(at, 8), pl.ds(0, 512)]
            cond = expanded[pl.ds(at, 8), pl.ds(512, 512)]
            for w in range(0, 8, 2):
                both_w = jnp.concatenate([val[w : w + 1] * cond, val[w + 1 : w + 2] * cond], 0)
                to = pl.multiple_of(c * 64 + w * 8, 16)
                rsm[pl.ds(to, 16), pl.ds(t * 512, 512)] = both_w.astype(BF16)
        return carry

    lax.fori_loop(0, CORNERS, rotate, 0)

    for p in range(8):
        blocks = []
        for ff in range(2):
            f = p * 2 + ff
            quads = []
            for q in range(4):
                a = left[off_l[f * CORNERS + 2 * q]]
                b = left[off_l[f * CORNERS + 2 * q + 1]]
                quads.append(jnp.where(near, a, b))
            blocks.append(jnp.concatenate(quads, axis=1))
        res = jnp.dot(
            jnp.concatenate(blocks, axis=0),
            rsm[:, p * 128 : (p + 1) * 128],
            preferred_element_type=F32,
        )
        turned = pltpu.roll(res, 64, 1)
        mixed[p * 128 : p * 128 + 64, :] = jnp.where(near, res[:64], turned[:64])
        mixed[p * 128 + 64 : p * 128 + 128, :] = jnp.where(near, turned[64:], res[64:])

    near_f = lanes((16, 128)) < 64
    for t in range(32):
        even = mixed[pl.ds(2 * t, 16, stride=64), :]
        odd = mixed[pl.ds(2 * t + 1, 16, stride=64), :]
        out[:, t * 128 : (t + 1) * 128] = jnp.where(near_f, even, odd).astype(BF16)

    upper.wait_send()

    def sent(d, carry):
        for way in range(2):
            for j in range(NC):
                wave(way, d, j).wait_send()

            @pl.when(d <= NEAR)
            def _():
                tile(way, d).wait_send()

        return carry

    lax.fori_loop(1, last + 1, sent, 0)
    for way in range(2):
        chosen_wave(way, True).wait_send()
        chosen_wave(way, False).wait_send()
        last_wave(way).wait_send()
        for k in range(NEAR + 1, half + 1):
            far_tile(way, k).wait_send()
    to_core.wait_send()
    for r in range(1, nx):
        to_x(r).wait_send()
    for r in range(1, ny):
        to_y(r).wait_send()
    across().wait_send()


def body(mesh_shape, *args):
    (fine_waves, coarse_waves, coarse_kernel, row_valence, row_conduction, row_neighbours,
     row_weight_index, col_neighbours, col_weight_index, tile_list, weight_table) = args
    nz, ng = mesh_shape
    nx = CORNERS // 2
    ny = ng // CORNERS
    width = fine_waves.shape[2]
    held = coarse_waves.shape[0]
    any_space = pl.BlockSpec(memory_space=pl.ANY)
    vmem = pl.BlockSpec(memory_space=pltpu.VMEM)
    smem = pl.BlockSpec(memory_space=pltpu.SMEM)
    half = nz // 2
    dma = pltpu.SemaphoreType.DMA
    out = pl.pallas_call(
        functools.partial(kernel, nz, nx, ny),
        out_shape=jax.ShapeDtypeStruct((16, PAIRS * PAIRS), BF16),
        in_specs=[any_space] * 3 + [vmem] * 2 + [smem] * 6,
        out_specs=vmem,
        scratch_shapes=[
            pltpu.VMEM((256, width), BF16),
            pltpu.VMEM((nz, held, BANDS, width), BF16),
            pltpu.VMEM((2, held, BANDS, width), BF16),
            pltpu.VMEM((nz * held * 2, 8, 256), F32),
            pltpu.VMEM((12, PAIRS, 512), BF16),
            pltpu.VMEM((2 * nz * 4, PAIRS, 128), BF16),
            pltpu.VMEM((2, 8, PAIRS, 128), BF16),
            pltpu.VMEM((128, 1024), BF16),
            pltpu.VMEM((128, 1024), F32),
            pltpu.VMEM((512, 1024), BF16),
            pltpu.VMEM((1024, 128), F32),
            pltpu.VMEM((2, SLOTS * 3 // 2, BANDS, width), BF16),
            pltpu.VMEM((2, half - NEAR, 2, PAIRS, 128), BF16),
            pltpu.VMEM((CORNERS, 8, 256), F32),
            pltpu.VMEM((nx, 8, 256), F32),
            pltpu.VMEM((nx, 8, 256), F32),
            pltpu.VMEM((nx - 1, nx, 8, 256), F32),
            pltpu.VMEM((nx, 8, 256), F32),
            pltpu.VMEM((ny - 1, nx, 8, 256), F32),
            pltpu.VMEM((CORNERS, 8, 256), F32),
            pltpu.SMEM((128,), jnp.int32),
            pltpu.SMEM((128,), jnp.int32),
            pltpu.SMEM((128,), F32),
            pltpu.SMEM((32,), jnp.int32),
            pltpu.SMEM((32,), jnp.int32),
            dma((3,)),
            dma((2, half, NC)),
            dma((2, half, NC)),
            dma,
            dma,
            dma((2, NEAR)),
            dma((2, NEAR)),
            dma((2, half - NEAR)),
            dma((2, half - NEAR)),
            dma((2,)),
            dma((2,)),
            dma((nx - 1,)),
            dma((nx - 1,)),
            dma((ny - 1,)),
            dma((ny - 1,)),
        ],
        compiler_params=pltpu.CompilerParams(
            collective_id=0, has_side_effects=True, vmem_limit_bytes=60 * 1024 * 1024
        ),
        name="interpolate",
    )(
        fine_waves.reshape(16 * BANDS, width),
        coarse_waves,
        coarse_kernel,
        row_valence.reshape(64, 8),
        row_conduction.reshape(64, 8),
        row_neighbours,
        row_weight_index,
        col_neighbours.T,
        col_weight_index.T,
        tile_list,
        weight_table,
    )
    return out[None]


def solution(mesh):
    placed = (
        P("ka", None, "ga"),
        P("ka", None, "ga"),
        P("ga", None, "ka"),
        P("ga", None, None, None),
        P("ga", None, None, None),
        P("ga", None),
        P("ga", None),
        P("ka", None),
        P("ka", None),
        P(),
        P(),
    )
    shape = (mesh.shape["ka"], mesh.shape["ga"])
    return jax.shard_map(
        functools.partial(body, shape),
        mesh=mesh,
        in_specs=placed,
        out_specs=P("ga", "ka", None),
        check_vma=False,
    )
```

```python
import functools
import math

import jax
import jax.numpy as jnp
from jax import lax
from jax.experimental import pallas as pl
from jax.experimental.pallas import tpu as pltpu
from jax.sharding import PartitionSpec as P

MESH = pl.DeviceIdType.MESH
PLANE_WAVES = 40960
CORNERS = 8
PAIRS = 64
BANDS = 16
F32 = jnp.float32
BF16 = jnp.bfloat16
NC = 2
NEAR = 5
SLOTS = 4


def lanes(shape):
    return lax.broadcasted_iota(jnp.int32, shape, len(shape) - 1)


def kernel(
    nz, nx, ny,
    fine_hbm, coarse_hbm, tiles_hbm, rv_hbm, rc_hbm, rn_hbm, rwi_hbm, cn_hbm, cwi_hbm, tl_hbm, wt_hbm,
    out,
    rv, rc, rn, rwi, cn, cwi, tl, wt,
    fine, waves, far_w, dense, stack, left, near_t, spread, expanded, rsm, mixed, picked_w, picked_t, sel, from_core,
    part, from_x, sum1, from_y, full, off_d, off_l, wgt, rank, first,
    in_sem, ws, wr, up_s, up_r, ts, tr, far_s, far_r, core_s, core_r, x_s, x_r, y_s, y_r,
):
    g, z = lax.axis_index("ga"), lax.axis_index("ka")
    ng = 2 * nx * ny
    half = nz // 2
    last = half - 2
    assert NEAR == last - 1
    piece = waves.shape[1] // NC
    core = lax.rem(g, 2)
    y, x = g // (2 * nx), lax.rem(g // 2, nx)
    partner = g + 1 - 2 * core

    def away(way, n):
        return lax.rem(z + (n if way == 0 else nz - n), nz)

    nbr = (away(0, 1), away(1, 1))

    get_coarse = pltpu.make_async_copy(coarse_hbm, waves.at[0], in_sem.at[0])
    get_tiles = pltpu.make_async_copy(tiles_hbm, stack.at[pl.ds(0, 6)], in_sem.at[1])
    get_fine = pltpu.make_async_copy(fine_hbm, fine, in_sem.at[2])
    get_coarse.start()
    get_tiles.start()
    get_fine.start()
    small = ((rv_hbm, rv), (rc_hbm, rc), (rn_hbm, rn), (rwi_hbm, rwi), (cn_hbm, cn), (cwi_hbm, cwi))
    small += ((tl_hbm, tl), (wt_hbm, wt))
    get_small = [
        pltpu.make_async_copy(src, dst, in_sem.at[3 + i]) for i, (src, dst) in enumerate(small)
    ]
    for copy in get_small:
        copy.start()

    def x_peer(r):
        return y * (2 * nx) + 2 * lax.rem(x + r, nx) + core

    def y_peer(r):
        return lax.rem(y + r, ny) * (2 * nx) + 2 * x + core

    up_to, up_from = lax.rem(g + ng - 1, ng), lax.rem(g + 1, ng)
    barrier = pltpu.get_barrier_semaphore()
    friends = [(g, away(way, n)) for n in range(1, half - NEAR + 1) for way in range(2)]
    friends += [(up_to, z), (up_from, z), (partner, z)]
    friends += [(x_peer(r), z) for r in range(1, nx)]
    friends += [(y_peer(r), z) for r in range(1, ny)]
    for who in friends:
        pl.semaphore_signal(barrier, inc=1, device_id=who, device_id_type=MESH)
    pl.semaphore_wait(barrier, len(friends))

    def slot(way, d):
        return lax.rem(nz - d, nz) if way == 0 else d

    def wave(way, d, j):
        cols = pl.ds(j * piece, piece)
        whole = waves.at[slot(way, d), cols]
        return pltpu.make_async_remote_copy(
            src_ref=waves.at[slot(way, d - 1), cols],
            dst_ref=far_w.at[way, cols] if isinstance(d, int) and d == last else whole,
            send_sem=ws.at[way, d - 1, j],
            recv_sem=wr.at[way, d - 1, j],
            device_id=(g, nbr[way]),
            device_id_type=MESH,
        )

    def chosen_wave(way, onward):
        cols = pl.ds(SLOTS, SLOTS // 2) if onward else pl.ds(0, SLOTS)
        j = 0 if onward else 1
        return pltpu.make_async_remote_copy(
            src_ref=picked_w.at[way, cols],
            dst_ref=waves.at[slot(way, half - 1), cols],
            send_sem=ws.at[way, half - 2, j],
            recv_sem=wr.at[way, half - 2, j],
            device_id=(g, nbr[way]),
            device_id_type=MESH,
        )

    def last_wave(way):
        return pltpu.make_async_remote_copy(
            src_ref=waves.at[slot(way, half - 1), pl.ds(SLOTS, SLOTS // 2)],
            dst_ref=waves.at[half, pl.ds(way * (SLOTS // 2), SLOTS // 2)],
            send_sem=ws.at[way, half - 1, 0],
            recv_sem=wr.at[way, half - 1, 0],
            device_id=(g, nbr[way]),
            device_id_type=MESH,
        )

    def tile(way, k):
        whole = left.at[pl.ds(slot(way, k) * 4, 4)]
        return pltpu.make_async_remote_copy(
            src_ref=left.at[pl.ds(slot(way, k - 1) * 4, 4)],
            dst_ref=near_t.at[way, pl.ds(0, 4)] if isinstance(k, int) and k == NEAR else whole,
            send_sem=ts.at[way, k - 1],
            recv_sem=tr.at[way, k - 1],
            device_id=(g, nbr[way]),
            device_id_type=MESH,
        )

    def far_tile(way, k):
        begin, count = (0, 2) if k < half else (way, 1)
        return pltpu.make_async_remote_copy(
            src_ref=picked_t.at[way, k - NEAR - 1, pl.ds(begin, count)],
            dst_ref=left.at[pl.ds(slot(way, k) * 4 + begin, count)],
            send_sem=far_s.at[way, k - NEAR - 1],
            recv_sem=far_r.at[way, k - NEAR - 1],
            device_id=(g, away(way, k - NEAR)),
            device_id_type=MESH,
        )

    def swap(base, count):
        for q in range(count):
            v = left[base + q].astype(F32)
            left[nz * 4 + base + q] = pltpu.roll(v, 64, 1).astype(BF16)

    def correlate(s, j, way=None):
        block = waves[s, pl.ds(j * 4, 4)] if way is None else far_w[way, pl.ds(j * 4, 4)]
        rows = block.reshape(4 * BANDS, waves.shape[3])
        both = lax.dot_general(
            rows, fine[...], (((1,), (1,)), ((), ())), preferred_element_type=F32
        )
        dense[pl.ds(s * 16 + j * 8, 8)] = both.reshape(8, 8, 256)

    get_coarse.wait()
    for jj in range(NC):
        for way in range(2):
            wave(way, 1, jj).start()
    get_tiles.wait()
    upper = pltpu.make_async_remote_copy(
        src_ref=stack.at[pl.ds(0, 6)],
        dst_ref=stack.at[pl.ds(6, 6)],
        send_sem=up_s,
        recv_sem=up_r,
        device_id=(up_to, z),
        device_id_type=MESH,
    )
    upper.start()
    get_fine.wait()
    for copy in get_small:
        copy.wait()
    for j in range(2):
        correlate(0, j)

    scale = 1.0 / (PLANE_WAVES * math.sqrt(PAIRS))

    def ranks(n, carry):
        before, count = carry
        holder = lax.shift_right_logical(tl[z, n], 3)
        count = jnp.where(holder == before, count + 1, 0)
        rank[n] = count
        return holder, count

    lax.fori_loop(0, tl.shape[1], ranks, (jnp.int32(-1), jnp.int32(0)))

    def place(i, carry):
        f, c = i // CORNERS, i % CORNERS
        n = cn[c, f]
        col = tl[z, n]
        s = (lax.shift_right_logical(col, 3) - z + nz) & (nz - 1)
        hops = jnp.minimum(s, nz - s)
        jj = jnp.where(hops > last, rank[n], col & 7)
        off_d[i] = (s * 8 + jj) * 2
        jj = jnp.where(hops > NEAR, rank[n], col & 7)
        off_l[i] = s * 4 + lax.shift_right_logical(jj, 1) + ((jj + c) & 1) * (nz * 4)
        wgt[i] = wt[cwi[c, f]] * scale
        return carry

    lax.fori_loop(0, 128, place, 0)

    into = lanes((128, 1024))
    row = lax.broadcasted_iota(jnp.int32, (128, 1024), 0)
    local = into % 512
    wanted = (local // 64) * 16 + jnp.where(into < 512, (local % 64) // 8, 8 + local % 8)
    spread[...] = jnp.where(row == wanted, 1.0, 0.0).astype(BF16)

    def wave_step(d):
        for jj in range(NC):
            for way in range(2):
                wave(way, d, jj).wait_recv()
                wave(way, d + 1, jj).start()
            if (jj + 1) * piece % 4 == 0:
                for way in range(2):
                    correlate(slot(way, d), (jj + 1) * piece // 4 - 1)

    wave_step(1)

    wide = lanes((8, PAIRS))
    low = lax.broadcasted_iota(jnp.int32, (8, PAIRS), 0)
    to_w = jnp.where(wide // 8 == low, 1.0, 0.0)
    to_y = jnp.where(wide % 8 == low, 1.0, 0.0)
    exact = lax.Precision.HIGHEST
    row_v = jnp.dot(rv[...], to_w, precision=exact, preferred_element_type=F32)
    row_c = jnp.dot(rc[...], to_y, precision=exact, preferred_element_type=F32)
    upper.wait_recv()
    rotated = jnp.zeros((PAIRS, stack.shape[2]), F32)
    for c in range(CORNERS):
        w = wt[rwi[0, c]]
        cond = row_c[c * 8 : c * 8 + 8]
        mat = jnp.concatenate(
            [row_v[c * 8 + v : c * 8 + v + 1] * cond for v in range(8)], axis=0
        )
        mat = (w * mat * (1.0 / math.sqrt(PAIRS))).astype(BF16)
        rotated += jnp.dot(mat, stack[rn[0, c]], preferred_element_type=F32)
    rotated = rotated.astype(BF16)
    for q in range(4):
        left[q] = rotated[:, q * 128 : (q + 1) * 128]
    swap(0, 4)

    def tile_step(k):
        for way in range(2):
            tile(way, k - 1).wait_recv()
        for way in range(2):
            tile(way, k).start()
        for way in range(2):
            swap(slot(way, k - 1) * 4, 4)

    served = []
    for way in range(2):
        served += [(away(way, n), away(1 - way, last)) for n in (1, 2)]
        served += [(away(way, n), away(1 - way, NEAR)) for n in range(1, half - NEAR + 1)]
    per_way = len(served) // 2

    def starts(n, counts):
        return tuple(
            count + jnp.where(lax.shift_right_logical(tl[o, n], 3) < h, 1, 0)
            for count, (o, h) in zip(counts, served)
        )

    counts = lax.fori_loop(0, tl.shape[1], starts, (jnp.int32(0),) * len(served))
    for i, count in enumerate(counts):
        first[i] = count

    def entry(i, k):
        return tl[served[i][0], jnp.minimum(first[i] + k, tl.shape[1] - 1)] & 7

    for way in range(2):
        tile(way, 1).start()

    def both(d, carry):
        wave_step(d)
        tile_step(d)
        return carry

    lax.fori_loop(2, NEAR, both, 0)
    wave_step(NEAR)
    tile_step(NEAR)
    for way in range(2):
        for jj in range(NC):
            wave(way, last, jj).wait_recv()
    near = lanes((64, 128)) < 64
    for way in range(2):
        for n, (owner, k) in enumerate(
            [(0, k) for k in range(SLOTS)] + [(1, way * 2), (1, way * 2 + 1)]
        ):
            picked_w[way, n] = far_w[way, entry(way * per_way + owner, k)]
    for way in range(2):
        chosen_wave(way, True).start()
    for way in range(2):
        chosen_wave(way, False).start()
    for way in range(2):
        for j in range(2):
            correlate(slot(way, last), j, way)

    for way in range(2):
        tile(way, NEAR).wait_recv()
    for way in range(2):
        s = slot(way, NEAR)
        for q in range(4):
            v = near_t[way, q]
            turned = pltpu.roll(v.astype(F32), 64, 1).astype(BF16)
            near_t[way, 4 + q] = turned
            left[s * 4 + q] = v
            left[nz * 4 + s * 4 + q] = turned
        for n in range(half - NEAR):
            for q in range(2):
                lo = entry(way * per_way + 2 + n, 2 * q)
                hi = entry(way * per_way + 2 + n, 2 * q + 1)
                a = near_t[way, lax.shift_right_logical(lo, 1) + (lo & 1) * 4]
                b = near_t[way, lax.shift_right_logical(hi, 1) + ((hi + 1) & 1) * 4]
                picked_t[way, n, q] = jnp.where(near, a, b)
    for way in range(2):
        chosen_wave(way, True).wait_recv()
        last_wave(way).start()
    for way in range(2):
        chosen_wave(way, False).wait_recv()
        correlate(slot(way, half - 1), 0)
    for way in range(2):
        last_wave(way).wait_recv()
    correlate(half, 0)

    for k in range(half, NEAR, -1):
        for way in range(2):
            far_tile(way, k).start()

    lane = lanes((8, 128))

    def pick(c, carry):
        for t in range(2):
            acc = jnp.zeros((8, 128), F32)
            for ff in range(8):
                i = (t * 8 + ff) * CORNERS + c
                val = dense[off_d[i], :, t * 128 : t * 128 + 128] * wgt[i]
                cond = dense[off_d[i] + 1, :, t * 128 : t * 128 + 128]
                acc = jnp.where(lane // 8 == 2 * ff, val, acc)
                acc = jnp.where(lane // 8 == 2 * ff + 1, cond, acc)
            sel[c, :, pl.ds(t * 128, 128)] = acc
        return carry

    lax.fori_loop(0, CORNERS, pick, 0)

    to_core = pltpu.make_async_remote_copy(
        src_ref=sel.at[pl.ds((1 - core) * nx, nx)],
        dst_ref=from_core,
        send_sem=core_s.at[0],
        recv_sem=core_r.at[0],
        device_id=(partner, z),
        device_id_type=MESH,
    )

    def to_x(r):
        return pltpu.make_async_remote_copy(
            src_ref=part,
            dst_ref=from_x.at[r - 1],
            send_sem=x_s.at[r - 1],
            recv_sem=x_r.at[r - 1],
            device_id=(x_peer(r), z),
            device_id_type=MESH,
        )

    def to_y(r):
        return pltpu.make_async_remote_copy(
            src_ref=sum1,
            dst_ref=from_y.at[r - 1],
            send_sem=y_s.at[r - 1],
            recv_sem=y_r.at[r - 1],
            device_id=(y_peer(r), z),
            device_id_type=MESH,
        )

    def across(arriving=False):
        mine = 1 - core if arriving else core
        return pltpu.make_async_remote_copy(
            src_ref=full.at[pl.ds(core * nx, nx)],
            dst_ref=full.at[pl.ds(mine * nx, nx)],
            send_sem=core_s.at[1],
            recv_sem=core_r.at[1],
            device_id=(partner, z),
            device_id_type=MESH,
        )

    to_core.start()
    to_core.wait_recv()
    total = sel[pl.ds(core * nx, nx)] + from_core[...]
    part[...] = total
    for r in range(1, nx):
        to_x(r).start()
    for r in range(1, nx):
        to_x(r).wait_recv()
        total += from_x[r - 1]
    sum1[...] = total
    for r in range(1, ny):
        to_y(r).start()
    for r in range(1, ny):
        to_y(r).wait_recv()
        total += from_y[r - 1]
    full[pl.ds(core * nx, nx)] = total
    across().start()
    for k in range(NEAR + 1, half):
        for way in range(2):
            far_tile(way, k).wait_recv()
            swap(slot(way, k) * 4, 2)
    for way in range(2):
        far_tile(way, half).wait_recv()
    swap(half * 4, 2)
    def rotations(side):
        rows = nx * 8
        corr = full[pl.ds(side * nx, nx)].reshape(rows, 256)
        corr = jnp.concatenate([corr[:, :128], corr[:, 128:]], axis=0)
        high = corr.astype(BF16)
        rest = (corr - high.astype(F32)).astype(BF16)
        expanded[...] = jnp.dot(high, spread[...], preferred_element_type=F32) + jnp.dot(
            rest, spread[...], preferred_element_type=F32
        )

        def rotate(c, carry):
            for t in range(2):
                at = pl.multiple_of(t * rows + c * 8, 8)
                val = expanded[pl.ds(at, 8), pl.ds(0, 512)]
                cond = expanded[pl.ds(at, 8), pl.ds(512, 512)]
                for w in range(0, 8, 2):
                    both_w = jnp.concatenate(
                        [val[w : w + 1] * cond, val[w + 1 : w + 2] * cond], 0
                    )
                    to = pl.multiple_of((side * nx + c) * 64 + w * 8, 16)
                    rsm[pl.ds(to, 16), pl.ds(t * 512, 512)] = both_w.astype(BF16)
            return carry

        lax.fori_loop(0, nx, rotate, 0)

    rotations(core)
    across(True).wait_recv()
    rotations(1 - core)

    for p in range(8):
        blocks = []
        for ff in range(2):
            f = p * 2 + ff
            quads = []
            for q in range(4):
                a = left[off_l[f * CORNERS + 2 * q]]
                b = left[off_l[f * CORNERS + 2 * q + 1]]
                quads.append(jnp.where(near, a, b))
            blocks.append(jnp.concatenate(quads, axis=1))
        res = jnp.dot(
            jnp.concatenate(blocks, axis=0),
            rsm[:, p * 128 : (p + 1) * 128],
            preferred_element_type=F32,
        )
        turned = pltpu.roll(res, 64, 1)
        mixed[p * 128 : p * 128 + 64, :] = jnp.where(near, res[:64], turned[:64])
        mixed[p * 128 + 64 : p * 128 + 128, :] = jnp.where(near, turned[64:], res[64:])

    near_f = lanes((16, 128)) < 64
    for t in range(32):
        even = mixed[pl.ds(2 * t, 16, stride=64), :]
        odd = mixed[pl.ds(2 * t + 1, 16, stride=64), :]
        out[:, t * 128 : (t + 1) * 128] = jnp.where(near_f, even, odd).astype(BF16)

    upper.wait_send()

    def sent(d, carry):
        for way in range(2):
            for j in range(NC):
                wave(way, d, j).wait_send()

            @pl.when(d <= NEAR)
            def _():
                tile(way, d).wait_send()

        return carry

    lax.fori_loop(1, last + 1, sent, 0)
    for way in range(2):
        chosen_wave(way, True).wait_send()
        chosen_wave(way, False).wait_send()
        last_wave(way).wait_send()
        for k in range(NEAR + 1, half + 1):
            far_tile(way, k).wait_send()
    to_core.wait_send()
    for r in range(1, nx):
        to_x(r).wait_send()
    for r in range(1, ny):
        to_y(r).wait_send()
    across().wait_send()


def body(mesh_shape, *args):
    (fine_waves, coarse_waves, coarse_kernel, row_valence, row_conduction, row_neighbours,
     row_weight_index, col_neighbours, col_weight_index, tile_list, weight_table) = args
    nz, ng = mesh_shape
    nx = CORNERS // 2
    ny = ng // CORNERS
    width = fine_waves.shape[2]
    held = coarse_waves.shape[0]
    any_space = pl.BlockSpec(memory_space=pl.ANY)
    vmem = pl.BlockSpec(memory_space=pltpu.VMEM)
    smem = pltpu.SMEM
    half = nz // 2
    dma = pltpu.SemaphoreType.DMA
    out = pl.pallas_call(
        functools.partial(kernel, nz, nx, ny),
        out_shape=jax.ShapeDtypeStruct((16, PAIRS * PAIRS), BF16),
        in_specs=[any_space] * 11,
        out_specs=vmem,
        scratch_shapes=[
            pltpu.VMEM((64, 8), F32),
            pltpu.VMEM((64, 8), F32),
            smem((1, CORNERS), jnp.int32),
            smem((1, CORNERS), jnp.int32),
            smem((CORNERS, 16), jnp.int32),
            smem((CORNERS, 16), jnp.int32),
            smem(tile_list.shape, jnp.int32),
            smem(weight_table.shape, F32),
            pltpu.VMEM((256, width), BF16),
            pltpu.VMEM((nz, held, BANDS, width), BF16),
            pltpu.VMEM((2, held, BANDS, width), BF16),
            pltpu.VMEM((nz * held * 2, 8, 256), F32),
            pltpu.VMEM((12, PAIRS, 512), BF16),
            pltpu.VMEM((2 * nz * 4, PAIRS, 128), BF16),
            pltpu.VMEM((2, 8, PAIRS, 128), BF16),
            pltpu.VMEM((128, 1024), BF16),
            pltpu.VMEM((64, 1024), F32),
            pltpu.VMEM((512, 1024), BF16),
            pltpu.VMEM((1024, 128), F32),
            pltpu.VMEM((2, SLOTS * 3 // 2, BANDS, width), BF16),
            pltpu.VMEM((2, half - NEAR, 2, PAIRS, 128), BF16),
            pltpu.VMEM((CORNERS, 8, 256), F32),
            pltpu.VMEM((nx, 8, 256), F32),
            pltpu.VMEM((nx, 8, 256), F32),
            pltpu.VMEM((nx - 1, nx, 8, 256), F32),
            pltpu.VMEM((nx, 8, 256), F32),
            pltpu.VMEM((ny - 1, nx, 8, 256), F32),
            pltpu.VMEM((CORNERS, 8, 256), F32),
            pltpu.SMEM((128,), jnp.int32),
            pltpu.SMEM((128,), jnp.int32),
            pltpu.SMEM((128,), F32),
            pltpu.SMEM((32,), jnp.int32),
            pltpu.SMEM((32,), jnp.int32),
            dma((11,)),
            dma((2, half, NC)),
            dma((2, half, NC)),
            dma,
            dma,
            dma((2, NEAR)),
            dma((2, NEAR)),
            dma((2, half - NEAR)),
            dma((2, half - NEAR)),
            dma((2,)),
            dma((2,)),
            dma((nx - 1,)),
            dma((nx - 1,)),
            dma((ny - 1,)),
            dma((ny - 1,)),
        ],
        compiler_params=pltpu.CompilerParams(
            collective_id=0, has_side_effects=True, vmem_limit_bytes=60 * 1024 * 1024
        ),
        name="interpolate",
    )(
        fine_waves.reshape(16 * BANDS, width),
        coarse_waves,
        coarse_kernel,
        row_valence.reshape(64, 8),
        row_conduction.reshape(64, 8),
        row_neighbours,
        row_weight_index,
        col_neighbours.T,
        col_weight_index.T,
        tile_list,
        weight_table,
    )
    return out[None]


def solution(mesh):
    placed = (
        P("ka", None, "ga"),
        P("ka", None, "ga"),
        P("ga", None, "ka"),
        P("ga", None, None, None),
        P("ga", None, None, None),
        P("ga", None),
        P("ga", None),
        P("ka", None),
        P("ka", None),
        P(),
        P(),
    )
    shape = (mesh.shape["ka"], mesh.shape["ga"])
    return jax.shard_map(
        functools.partial(body, shape),
        mesh=mesh,
        in_specs=placed,
        out_specs=P("ga", "ka", None),
        check_vma=False,
    )
```

```python
import functools
import math

import jax
import jax.numpy as jnp
from jax import lax
from jax.experimental import pallas as pl
from jax.experimental.pallas import tpu as pltpu
from jax.sharding import PartitionSpec as P

MESH = pl.DeviceIdType.MESH
PLANE_WAVES = 40960
CORNERS = 8
PAIRS = 64
BANDS = 16
F32 = jnp.float32
BF16 = jnp.bfloat16
NC = 2
NEAR = 5
SLOTS = 4


def lanes(shape):
    return lax.broadcasted_iota(jnp.int32, shape, len(shape) - 1)


def kernel(
    nz, nx, ny,
    fine_hbm, coarse_hbm, tiles_hbm, rv_hbm, rc_hbm, rn_hbm, rwi_hbm, cn_hbm, cwi_hbm, tl_hbm, wt_hbm,
    out,
    rv, rc, rn, rwi, cn, cwi, tl, wt,
    fine, waves, far_w, dense, stack, left, near_t, spread, expanded, rsm, mixed, picked_w, picked_t, sel, from_core,
    part, from_x, sum1, from_y, full, off_d, off_l, wgt, rank, first,
    in_sem, ws, wr, up_s, up_r, ts, tr, far_s, far_r, core_s, core_r, x_s, x_r, y_s, y_r, word,
):
    g, z = lax.axis_index("ga"), lax.axis_index("ka")
    ng = 2 * nx * ny
    half = nz // 2
    last = half - 2
    assert NEAR == last - 1
    piece = waves.shape[1] // NC
    core = lax.rem(g, 2)
    y, x = g // (2 * nx), lax.rem(g // 2, nx)
    partner = g + 1 - 2 * core

    def away(way, n):
        return lax.rem(z + (n if way == 0 else nz - n), nz)

    nbr = (away(0, 1), away(1, 1))

    get_coarse = pltpu.make_async_copy(coarse_hbm, waves.at[0], in_sem.at[0])
    get_tiles = pltpu.make_async_copy(tiles_hbm, stack.at[pl.ds(0, 6)], in_sem.at[1])
    get_fine = pltpu.make_async_copy(fine_hbm, fine, in_sem.at[2])
    get_coarse.start()
    get_tiles.start()
    get_fine.start()
    small = ((rv_hbm, rv), (rc_hbm, rc), (rn_hbm, rn), (rwi_hbm, rwi), (cn_hbm, cn), (cwi_hbm, cwi))
    small += ((tl_hbm, tl), (wt_hbm, wt))
    get_small = [
        pltpu.make_async_copy(src, dst, in_sem.at[3 + i]) for i, (src, dst) in enumerate(small)
    ]
    for copy in get_small:
        copy.start()

    def x_peer(r):
        return y * (2 * nx) + 2 * lax.rem(x + r, nx) + core

    def y_peer(r):
        return lax.rem(y + r, ny) * (2 * nx) + 2 * x + core

    up_to, up_from = lax.rem(g + ng - 1, ng), lax.rem(g + 1, ng)
    barrier = pltpu.get_barrier_semaphore()
    friends = [(g, nbr[0]), (g, nbr[1]), (up_to, z), (up_from, z)]
    for who in friends:
        pl.semaphore_signal(barrier, inc=1, device_id=who, device_id_type=MESH)
    pl.semaphore_wait(barrier, len(friends))

    steps = ((1, 0), (2, 0), (4, 0), (8, 0), (0, 1), (0, 1))

    def pass_word(i):
        by_g, by_z = steps[i]
        for sign in (1, -1):
            who = (lax.rem(g + sign * by_g + ng, ng), lax.rem(z + sign * by_z + nz, nz))
            pl.semaphore_signal(word.at[i], inc=1, device_id=who, device_id_type=MESH)

    def hear_word(i):
        pl.semaphore_wait(word.at[i], 2)

    def slot(way, d):
        return lax.rem(nz - d, nz) if way == 0 else d

    def wave(way, d, j):
        cols = pl.ds(j * piece, piece)
        whole = waves.at[slot(way, d), cols]
        return pltpu.make_async_remote_copy(
            src_ref=waves.at[slot(way, d - 1), cols],
            dst_ref=far_w.at[way, cols] if isinstance(d, int) and d == last else whole,
            send_sem=ws.at[way, d - 1, j],
            recv_sem=wr.at[way, d - 1, j],
            device_id=(g, nbr[way]),
            device_id_type=MESH,
        )

    def chosen_wave(way, onward):
        cols = pl.ds(SLOTS, SLOTS // 2) if onward else pl.ds(0, SLOTS)
        j = 0 if onward else 1
        return pltpu.make_async_remote_copy(
            src_ref=picked_w.at[way, cols],
            dst_ref=waves.at[slot(way, half - 1), cols],
            send_sem=ws.at[way, half - 2, j],
            recv_sem=wr.at[way, half - 2, j],
            device_id=(g, nbr[way]),
            device_id_type=MESH,
        )

    def last_wave(way):
        return pltpu.make_async_remote_copy(
            src_ref=waves.at[slot(way, half - 1), pl.ds(SLOTS, SLOTS // 2)],
            dst_ref=waves.at[half, pl.ds(way * (SLOTS // 2), SLOTS // 2)],
            send_sem=ws.at[way, half - 1, 0],
            recv_sem=wr.at[way, half - 1, 0],
            device_id=(g, nbr[way]),
            device_id_type=MESH,
        )

    def tile(way, k):
        whole = left.at[pl.ds(slot(way, k) * 4, 4)]
        return pltpu.make_async_remote_copy(
            src_ref=left.at[pl.ds(slot(way, k - 1) * 4, 4)],
            dst_ref=near_t.at[way, pl.ds(0, 4)] if isinstance(k, int) and k == NEAR else whole,
            send_sem=ts.at[way, k - 1],
            recv_sem=tr.at[way, k - 1],
            device_id=(g, nbr[way]),
            device_id_type=MESH,
        )

    def far_tile(way, k):
        begin, count = (0, 2) if k < half else (way, 1)
        return pltpu.make_async_remote_copy(
            src_ref=picked_t.at[way, k - NEAR - 1, pl.ds(begin, count)],
            dst_ref=left.at[pl.ds(slot(way, k) * 4 + begin, count)],
            send_sem=far_s.at[way, k - NEAR - 1],
            recv_sem=far_r.at[way, k - NEAR - 1],
            device_id=(g, away(way, k - NEAR)),
            device_id_type=MESH,
        )

    def swap(base, count):
        for q in range(count):
            v = left[base + q].astype(F32)
            left[nz * 4 + base + q] = pltpu.roll(v, 64, 1).astype(BF16)

    def correlate(s, j, way=None):
        block = waves[s, pl.ds(j * 4, 4)] if way is None else far_w[way, pl.ds(j * 4, 4)]
        rows = block.reshape(4 * BANDS, waves.shape[3])
        both = lax.dot_general(
            rows, fine[...], (((1,), (1,)), ((), ())), preferred_element_type=F32
        )
        dense[pl.ds(s * 16 + j * 8, 8)] = both.reshape(8, 8, 256)

    get_coarse.wait()
    for jj in range(NC):
        for way in range(2):
            wave(way, 1, jj).start()
    pass_word(0)
    pass_word(4)
    get_tiles.wait()
    upper = pltpu.make_async_remote_copy(
        src_ref=stack.at[pl.ds(0, 6)],
        dst_ref=stack.at[pl.ds(6, 6)],
        send_sem=up_s,
        recv_sem=up_r,
        device_id=(up_to, z),
        device_id_type=MESH,
    )
    upper.start()
    get_fine.wait()
    for copy in get_small:
        copy.wait()
    for j in range(2):
        correlate(0, j)

    scale = 1.0 / (PLANE_WAVES * math.sqrt(PAIRS))

    def ranks(n, carry):
        before, count = carry
        holder = lax.shift_right_logical(tl[z, n], 3)
        count = jnp.where(holder == before, count + 1, 0)
        rank[n] = count
        return holder, count

    lax.fori_loop(0, tl.shape[1], ranks, (jnp.int32(-1), jnp.int32(0)))

    def place(i, carry):
        f, c = i // CORNERS, i % CORNERS
        n = cn[c, f]
        col = tl[z, n]
        s = (lax.shift_right_logical(col, 3) - z + nz) & (nz - 1)
        hops = jnp.minimum(s, nz - s)
        jj = jnp.where(hops > last, rank[n], col & 7)
        off_d[i] = (s * 8 + jj) * 2
        jj = jnp.where(hops > NEAR, rank[n], col & 7)
        off_l[i] = s * 4 + lax.shift_right_logical(jj, 1) + ((jj + c) & 1) * (nz * 4)
        wgt[i] = wt[cwi[c, f]] * scale
        return carry

    lax.fori_loop(0, 128, place, 0)

    into = lanes((128, 1024))
    row = lax.broadcasted_iota(jnp.int32, (128, 1024), 0)
    local = into % 512
    wanted = (local // 64) * 16 + jnp.where(into < 512, (local % 64) // 8, 8 + local % 8)
    spread[...] = jnp.where(row == wanted, 1.0, 0.0).astype(BF16)

    def wave_step(d):
        for jj in range(NC):
            for way in range(2):
                wave(way, d, jj).wait_recv()
                wave(way, d + 1, jj).start()
            if (jj + 1) * piece % 4 == 0:
                for way in range(2):
                    correlate(slot(way, d), (jj + 1) * piece // 4 - 1)

    hear_word(0)
    hear_word(4)
    pass_word(1)
    pass_word(5)
    wave_step(1)

    wide = lanes((8, PAIRS))
    low = lax.broadcasted_iota(jnp.int32, (8, PAIRS), 0)
    to_w = jnp.where(wide // 8 == low, 1.0, 0.0)
    to_y = jnp.where(wide % 8 == low, 1.0, 0.0)
    exact = lax.Precision.HIGHEST
    row_v = jnp.dot(rv[...], to_w, precision=exact, preferred_element_type=F32)
    row_c = jnp.dot(rc[...], to_y, precision=exact, preferred_element_type=F32)
    upper.wait_recv()
    rotated = jnp.zeros((PAIRS, stack.shape[2]), F32)
    for c in range(CORNERS):
        w = wt[rwi[0, c]]
        cond = row_c[c * 8 : c * 8 + 8]
        mat = jnp.concatenate(
            [row_v[c * 8 + v : c * 8 + v + 1] * cond for v in range(8)], axis=0
        )
        mat = (w * mat * (1.0 / math.sqrt(PAIRS))).astype(BF16)
        rotated += jnp.dot(mat, stack[rn[0, c]], preferred_element_type=F32)
    rotated = rotated.astype(BF16)
    for q in range(4):
        left[q] = rotated[:, q * 128 : (q + 1) * 128]
    swap(0, 4)

    def tile_step(k):
        for way in range(2):
            tile(way, k - 1).wait_recv()
        for way in range(2):
            tile(way, k).start()
        for way in range(2):
            swap(slot(way, k - 1) * 4, 4)

    served = []
    for way in range(2):
        served += [(away(way, n), away(1 - way, last)) for n in (1, 2)]
        served += [(away(way, n), away(1 - way, NEAR)) for n in range(1, half - NEAR + 1)]
    per_way = len(served) // 2

    def starts(n, counts):
        return tuple(
            count + jnp.where(lax.shift_right_logical(tl[o, n], 3) < h, 1, 0)
            for count, (o, h) in zip(counts, served)
        )

    counts = lax.fori_loop(0, tl.shape[1], starts, (jnp.int32(0),) * len(served))
    for i, count in enumerate(counts):
        first[i] = count

    def entry(i, k):
        return tl[served[i][0], jnp.minimum(first[i] + k, tl.shape[1] - 1)] & 7

    for way in range(2):
        tile(way, 1).start()

    def both(d, carry):
        wave_step(d)
        tile_step(d)
        return carry

    hear_word(1)
    hear_word(5)
    pass_word(2)
    lax.fori_loop(2, NEAR, both, 0)
    hear_word(2)
    pass_word(3)
    wave_step(NEAR)
    tile_step(NEAR)
    hear_word(3)
    for way in range(2):
        for jj in range(NC):
            wave(way, last, jj).wait_recv()
    near = lanes((64, 128)) < 64
    for way in range(2):
        for n, (owner, k) in enumerate(
            [(0, k) for k in range(SLOTS)] + [(1, way * 2), (1, way * 2 + 1)]
        ):
            picked_w[way, n] = far_w[way, entry(way * per_way + owner, k)]
    for way in range(2):
        chosen_wave(way, True).start()
    for way in range(2):
        chosen_wave(way, False).start()
    for way in range(2):
        for j in range(2):
            correlate(slot(way, last), j, way)

    for way in range(2):
        tile(way, NEAR).wait_recv()
    for way in range(2):
        s = slot(way, NEAR)
        for q in range(4):
            v = near_t[way, q]
            turned = pltpu.roll(v.astype(F32), 64, 1).astype(BF16)
            near_t[way, 4 + q] = turned
            left[s * 4 + q] = v
            left[nz * 4 + s * 4 + q] = turned
        for n in range(half - NEAR):
            for q in range(2):
                lo = entry(way * per_way + 2 + n, 2 * q)
                hi = entry(way * per_way + 2 + n, 2 * q + 1)
                a = near_t[way, lax.shift_right_logical(lo, 1) + (lo & 1) * 4]
                b = near_t[way, lax.shift_right_logical(hi, 1) + ((hi + 1) & 1) * 4]
                picked_t[way, n, q] = jnp.where(near, a, b)
    for way in range(2):
        chosen_wave(way, True).wait_recv()
        last_wave(way).start()
    for way in range(2):
        chosen_wave(way, False).wait_recv()
        correlate(slot(way, half - 1), 0)
    for way in range(2):
        last_wave(way).wait_recv()
    correlate(half, 0)

    for k in range(half, NEAR, -1):
        for way in range(2):
            far_tile(way, k).start()

    lane = lanes((8, 128))

    def pick(i, side):
        c = side * nx + i
        for t in range(2):
            acc = jnp.zeros((8, 128), F32)
            for ff in range(8):
                n = (t * 8 + ff) * CORNERS + c
                val = dense[off_d[n], :, t * 128 : t * 128 + 128] * wgt[n]
                cond = dense[off_d[n] + 1, :, t * 128 : t * 128 + 128]
                acc = jnp.where(lane // 8 == 2 * ff, val, acc)
                acc = jnp.where(lane // 8 == 2 * ff + 1, cond, acc)
            sel[c, :, pl.ds(t * 128, 128)] = acc
        return side

    lax.fori_loop(0, nx, pick, 1 - core)

    to_core = pltpu.make_async_remote_copy(
        src_ref=sel.at[pl.ds((1 - core) * nx, nx)],
        dst_ref=from_core,
        send_sem=core_s.at[0],
        recv_sem=core_r.at[0],
        device_id=(partner, z),
        device_id_type=MESH,
    )

    def to_x(r):
        return pltpu.make_async_remote_copy(
            src_ref=part,
            dst_ref=from_x.at[r - 1],
            send_sem=x_s.at[r - 1],
            recv_sem=x_r.at[r - 1],
            device_id=(x_peer(r), z),
            device_id_type=MESH,
        )

    def to_y(r):
        return pltpu.make_async_remote_copy(
            src_ref=sum1,
            dst_ref=from_y.at[r - 1],
            send_sem=y_s.at[r - 1],
            recv_sem=y_r.at[r - 1],
            device_id=(y_peer(r), z),
            device_id_type=MESH,
        )

    def across(arriving=False):
        mine = 1 - core if arriving else core
        return pltpu.make_async_remote_copy(
            src_ref=full.at[pl.ds(core * nx, nx)],
            dst_ref=full.at[pl.ds(mine * nx, nx)],
            send_sem=core_s.at[1],
            recv_sem=core_r.at[1],
            device_id=(partner, z),
            device_id_type=MESH,
        )

    to_core.start()
    lax.fori_loop(0, nx, pick, core)
    to_core.wait_recv()
    total = sel[pl.ds(core * nx, nx)] + from_core[...]
    part[...] = total
    for r in range(1, nx):
        to_x(r).start()
    for r in range(1, nx):
        to_x(r).wait_recv()
        total += from_x[r - 1]
    sum1[...] = total
    for r in range(1, ny):
        to_y(r).start()
    for r in range(1, ny):
        to_y(r).wait_recv()
        total += from_y[r - 1]
    full[pl.ds(core * nx, nx)] = total
    across().start()
    for k in range(NEAR + 1, half):
        for way in range(2):
            far_tile(way, k).wait_recv()
            swap(slot(way, k) * 4, 2)
    for way in range(2):
        far_tile(way, half).wait_recv()
    swap(half * 4, 2)
    def rotations(side):
        rows = nx * 8
        corr = full[pl.ds(side * nx, nx)].reshape(rows, 256)
        corr = jnp.concatenate([corr[:, :128], corr[:, 128:]], axis=0)
        high = corr.astype(BF16)
        rest = (corr - high.astype(F32)).astype(BF16)
        expanded[...] = jnp.dot(high, spread[...], preferred_element_type=F32) + jnp.dot(
            rest, spread[...], preferred_element_type=F32
        )

        def rotate(c, carry):
            for t in range(2):
                at = pl.multiple_of(t * rows + c * 8, 8)
                val = expanded[pl.ds(at, 8), pl.ds(0, 512)]
                cond = expanded[pl.ds(at, 8), pl.ds(512, 512)]
                for w in range(0, 8, 2):
                    both_w = jnp.concatenate(
                        [val[w : w + 1] * cond, val[w + 1 : w + 2] * cond], 0
                    )
                    to = pl.multiple_of((side * nx + c) * 64 + w * 8, 16)
                    rsm[pl.ds(to, 16), pl.ds(t * 512, 512)] = both_w.astype(BF16)
            return carry

        lax.fori_loop(0, nx, rotate, 0)

    def products(side, add):
        for p in range(8):
            blocks = []
            for ff in range(2):
                at = (p * 2 + ff) * CORNERS + side * nx
                quads = []
                for q in range(2):
                    a, b = left[off_l[at + 2 * q]], left[off_l[at + 2 * q + 1]]
                    quads.append(jnp.where(near, a, b))
                blocks.append(jnp.concatenate(quads, axis=1))
            res = jnp.dot(
                jnp.concatenate(blocks, axis=0),
                rsm[pl.ds(side * 256, 256), p * 128 : (p + 1) * 128],
                preferred_element_type=F32,
            )
            if add:
                res += mixed[p * 128 : (p + 1) * 128]
                turned = pltpu.roll(res, 64, 1)
                even = jnp.where(near, res[:64], turned[:64])
                odd = jnp.where(near, turned[64:], res[64:])
                res = jnp.concatenate([even, odd], axis=0)
            mixed[p * 128 : (p + 1) * 128] = res

    rotations(core)
    products(core, False)
    across(True).wait_recv()
    rotations(1 - core)
    products(1 - core, True)

    near_f = lanes((16, 128)) < 64
    for t in range(32):
        even = mixed[pl.ds(2 * t, 16, stride=64), :]
        odd = mixed[pl.ds(2 * t + 1, 16, stride=64), :]
        out[:, t * 128 : (t + 1) * 128] = jnp.where(near_f, even, odd).astype(BF16)

    upper.wait_send()

    def sent(d, carry):
        for way in range(2):
            for j in range(NC):
                wave(way, d, j).wait_send()

            @pl.when(d <= NEAR)
            def _():
                tile(way, d).wait_send()

        return carry

    lax.fori_loop(1, last + 1, sent, 0)
    for way in range(2):
        chosen_wave(way, True).wait_send()
        chosen_wave(way, False).wait_send()
        last_wave(way).wait_send()
        for k in range(NEAR + 1, half + 1):
            far_tile(way, k).wait_send()
    to_core.wait_send()
    for r in range(1, nx):
        to_x(r).wait_send()
    for r in range(1, ny):
        to_y(r).wait_send()
    across().wait_send()


def body(mesh_shape, *args):
    (fine_waves, coarse_waves, coarse_kernel, row_valence, row_conduction, row_neighbours,
     row_weight_index, col_neighbours, col_weight_index, tile_list, weight_table) = args
    nz, ng = mesh_shape
    nx = CORNERS // 2
    ny = ng // CORNERS
    width = fine_waves.shape[2]
    held = coarse_waves.shape[0]
    any_space = pl.BlockSpec(memory_space=pl.ANY)
    vmem = pl.BlockSpec(memory_space=pltpu.VMEM)
    smem = pltpu.SMEM
    half = nz // 2
    dma = pltpu.SemaphoreType.DMA
    out = pl.pallas_call(
        functools.partial(kernel, nz, nx, ny),
        out_shape=jax.ShapeDtypeStruct((16, PAIRS * PAIRS), BF16),
        in_specs=[any_space] * 11,
        out_specs=vmem,
        scratch_shapes=[
            pltpu.VMEM((64, 8), F32),
            pltpu.VMEM((64, 8), F32),
            smem((1, CORNERS), jnp.int32),
            smem((1, CORNERS), jnp.int32),
            smem((CORNERS, 16), jnp.int32),
            smem((CORNERS, 16), jnp.int32),
            smem(tile_list.shape, jnp.int32),
            smem(weight_table.shape, F32),
            pltpu.VMEM((256, width), BF16),
            pltpu.VMEM((nz, held, BANDS, width), BF16),
            pltpu.VMEM((2, held, BANDS, width), BF16),
            pltpu.VMEM((nz * held * 2, 8, 256), F32),
            pltpu.VMEM((12, PAIRS, 512), BF16),
            pltpu.VMEM((2 * nz * 4, PAIRS, 128), BF16),
            pltpu.VMEM((2, 8, PAIRS, 128), BF16),
            pltpu.VMEM((128, 1024), BF16),
            pltpu.VMEM((64, 1024), F32),
            pltpu.VMEM((512, 1024), BF16),
            pltpu.VMEM((1024, 128), F32),
            pltpu.VMEM((2, SLOTS * 3 // 2, BANDS, width), BF16),
            pltpu.VMEM((2, half - NEAR, 2, PAIRS, 128), BF16),
            pltpu.VMEM((CORNERS, 8, 256), F32),
            pltpu.VMEM((nx, 8, 256), F32),
            pltpu.VMEM((nx, 8, 256), F32),
            pltpu.VMEM((nx - 1, nx, 8, 256), F32),
            pltpu.VMEM((nx, 8, 256), F32),
            pltpu.VMEM((ny - 1, nx, 8, 256), F32),
            pltpu.VMEM((CORNERS, 8, 256), F32),
            pltpu.SMEM((128,), jnp.int32),
            pltpu.SMEM((128,), jnp.int32),
            pltpu.SMEM((128,), F32),
            pltpu.SMEM((32,), jnp.int32),
            pltpu.SMEM((32,), jnp.int32),
            dma((11,)),
            dma((2, half, NC)),
            dma((2, half, NC)),
            dma,
            dma,
            dma((2, NEAR)),
            dma((2, NEAR)),
            dma((2, half - NEAR)),
            dma((2, half - NEAR)),
            dma((2,)),
            dma((2,)),
            dma((nx - 1,)),
            dma((nx - 1,)),
            dma((ny - 1,)),
            dma((ny - 1,)),
            pltpu.SemaphoreType.REGULAR((6,)),
        ],
        compiler_params=pltpu.CompilerParams(
            collective_id=0, has_side_effects=True, vmem_limit_bytes=60 * 1024 * 1024
        ),
        name="interpolate",
    )(
        fine_waves.reshape(16 * BANDS, width),
        coarse_waves,
        coarse_kernel,
        row_valence.reshape(64, 8),
        row_conduction.reshape(64, 8),
        row_neighbours,
        row_weight_index,
        col_neighbours.T,
        col_weight_index.T,
        tile_list,
        weight_table,
    )
    return out[None]


def solution(mesh):
    placed = (
        P("ka", None, "ga"),
        P("ka", None, "ga"),
        P("ga", None, "ka"),
        P("ga", None, None, None),
        P("ga", None, None, None),
        P("ga", None),
        P("ga", None),
        P("ka", None),
        P("ka", None),
        P(),
        P(),
    )
    shape = (mesh.shape["ka"], mesh.shape["ga"])
    return jax.shard_map(
        functools.partial(body, shape),
        mesh=mesh,
        in_specs=placed,
        out_specs=P("ga", "ka", None),
        check_vma=False,
    )
```

```python
import functools
import math

import jax
import jax.numpy as jnp
from jax import lax
from jax.experimental import pallas as pl
from jax.experimental.pallas import tpu as pltpu
from jax.sharding import PartitionSpec as P

MESH = pl.DeviceIdType.MESH
PLANE_WAVES = 40960
CORNERS = 8
PAIRS = 64
BANDS = 16
F32 = jnp.float32
BF16 = jnp.bfloat16
NC = 2
NEAR = 5
SLOTS = 4


def lanes(shape):
    return lax.broadcasted_iota(jnp.int32, shape, len(shape) - 1)


def kernel(
    nz, nx, ny,
    fine_hbm, coarse_hbm, tiles_hbm, rv_hbm, rc_hbm, rn_hbm, rwi_hbm, cn_hbm, cwi_hbm, tl_hbm, wt_hbm,
    out_hbm,
    out, rv, rc, rn, rwi, cn, cwi, tl, wt,
    fine, waves, far_w, dense, stack, left, near_t, spread, expanded, rsm, mixed, picked_w, picked_t, sel, from_core,
    part, from_x, sum1, from_y, full, off_d, off_l, wgt, rank, first,
    in_sem, ws, wr, up_s, up_r, ts, tr, far_s, far_r, core_s, core_r, x_s, x_r, y_s, y_r, word,
):
    g, z = lax.axis_index("ga"), lax.axis_index("ka")
    ng = 2 * nx * ny
    half = nz // 2
    last = half - 2
    assert NEAR == last - 1
    piece = waves.shape[1] // NC
    core = lax.rem(g, 2)
    y, x = g // (2 * nx), lax.rem(g // 2, nx)
    partner = g + 1 - 2 * core

    def away(way, n):
        return lax.rem(z + (n if way == 0 else nz - n), nz)

    nbr = (away(0, 1), away(1, 1))

    get_coarse = pltpu.make_async_copy(coarse_hbm, waves.at[0], in_sem.at[0])
    get_tiles = pltpu.make_async_copy(tiles_hbm, stack.at[pl.ds(0, 6)], in_sem.at[1])
    get_fine = pltpu.make_async_copy(fine_hbm, fine, in_sem.at[2])
    get_coarse.start()
    get_tiles.start()
    get_fine.start()
    small = ((rv_hbm, rv), (rc_hbm, rc), (rn_hbm, rn), (rwi_hbm, rwi), (cn_hbm, cn), (cwi_hbm, cwi))
    small += ((tl_hbm, tl), (wt_hbm, wt))
    get_small = [
        pltpu.make_async_copy(src, dst, in_sem.at[3 + i]) for i, (src, dst) in enumerate(small)
    ]
    for copy in get_small:
        copy.start()

    def x_peer(r):
        return y * (2 * nx) + 2 * lax.rem(x + r, nx) + core

    def y_peer(r):
        return lax.rem(y + r, ny) * (2 * nx) + 2 * x + core

    up_to, up_from = lax.rem(g + ng - 1, ng), lax.rem(g + 1, ng)
    barrier = pltpu.get_barrier_semaphore()
    friends = [(g, nbr[0]), (g, nbr[1]), (up_to, z), (up_from, z)]
    for who in friends:
        pl.semaphore_signal(barrier, inc=1, device_id=who, device_id_type=MESH)
    pl.semaphore_wait(barrier, len(friends))

    steps = ((1, 0), (2, 0), (4, 0), (8, 0), (0, 1), (0, 1))

    def pass_word(i):
        by_g, by_z = steps[i]
        for sign in (1, -1):
            who = (lax.rem(g + sign * by_g + ng, ng), lax.rem(z + sign * by_z + nz, nz))
            pl.semaphore_signal(word.at[i], inc=1, device_id=who, device_id_type=MESH)

    def hear_word(i):
        pl.semaphore_wait(word.at[i], 2)

    def slot(way, d):
        return lax.rem(nz - d, nz) if way == 0 else d

    def wave(way, d, j):
        cols = pl.ds(j * piece, piece)
        whole = waves.at[slot(way, d), cols]
        return pltpu.make_async_remote_copy(
            src_ref=waves.at[slot(way, d - 1), cols],
            dst_ref=far_w.at[way, cols] if isinstance(d, int) and d == last else whole,
            send_sem=ws.at[way, d - 1, j],
            recv_sem=wr.at[way, d - 1, j],
            device_id=(g, nbr[way]),
            device_id_type=MESH,
        )

    def chosen_wave(way, onward):
        cols = pl.ds(SLOTS, SLOTS // 2) if onward else pl.ds(0, SLOTS)
        j = 0 if onward else 1
        return pltpu.make_async_remote_copy(
            src_ref=picked_w.at[way, cols],
            dst_ref=waves.at[slot(way, half - 1), cols],
            send_sem=ws.at[way, half - 2, j],
            recv_sem=wr.at[way, half - 2, j],
            device_id=(g, nbr[way]),
            device_id_type=MESH,
        )

    def last_wave(way):
        return pltpu.make_async_remote_copy(
            src_ref=waves.at[slot(way, half - 1), pl.ds(SLOTS, SLOTS // 2)],
            dst_ref=waves.at[half, pl.ds(way * (SLOTS // 2), SLOTS // 2)],
            send_sem=ws.at[way, half - 1, 0],
            recv_sem=wr.at[way, half - 1, 0],
            device_id=(g, nbr[way]),
            device_id_type=MESH,
        )

    def tile(way, k):
        whole = left.at[pl.ds(slot(way, k) * 4, 4)]
        return pltpu.make_async_remote_copy(
            src_ref=left.at[pl.ds(slot(way, k - 1) * 4, 4)],
            dst_ref=near_t.at[way, pl.ds(0, 4)] if isinstance(k, int) and k == NEAR else whole,
            send_sem=ts.at[way, k - 1],
            recv_sem=tr.at[way, k - 1],
            device_id=(g, nbr[way]),
            device_id_type=MESH,
        )

    def far_tile(way, k):
        begin, count = (0, 2) if k < half else (way, 1)
        return pltpu.make_async_remote_copy(
            src_ref=picked_t.at[way, k - NEAR - 1, pl.ds(begin, count)],
            dst_ref=left.at[pl.ds(slot(way, k) * 4 + begin, count)],
            send_sem=far_s.at[way, k - NEAR - 1],
            recv_sem=far_r.at[way, k - NEAR - 1],
            device_id=(g, away(way, k - NEAR)),
            device_id_type=MESH,
        )

    def swap(base, count):
        for q in range(count):
            v = left[base + q].astype(F32)
            left[nz * 4 + base + q] = pltpu.roll(v, 64, 1).astype(BF16)

    def correlate(s, j, way=None):
        block = waves[s, pl.ds(j * 4, 4)] if way is None else far_w[way, pl.ds(j * 4, 4)]
        rows = block.reshape(4 * BANDS, waves.shape[3])
        both = lax.dot_general(
            rows, fine[...], (((1,), (1,)), ((), ())), preferred_element_type=F32
        )
        dense[pl.ds(s * 16 + j * 8, 8)] = both.reshape(8, 8, 256)

    get_coarse.wait()
    for jj in range(NC):
        for way in range(2):
            wave(way, 1, jj).start()
    pass_word(0)
    pass_word(4)
    get_tiles.wait()
    upper = pltpu.make_async_remote_copy(
        src_ref=stack.at[pl.ds(0, 6)],
        dst_ref=stack.at[pl.ds(6, 6)],
        send_sem=up_s,
        recv_sem=up_r,
        device_id=(up_to, z),
        device_id_type=MESH,
    )
    upper.start()
    get_fine.wait()
    for copy in get_small:
        copy.wait()
    for j in range(2):
        correlate(0, j)

    scale = 1.0 / (PLANE_WAVES * math.sqrt(PAIRS))

    def ranks(n, carry):
        before, count = carry
        holder = lax.shift_right_logical(tl[z, n], 3)
        count = jnp.where(holder == before, count + 1, 0)
        rank[n] = count
        return holder, count

    lax.fori_loop(0, tl.shape[1], ranks, (jnp.int32(-1), jnp.int32(0)))

    def place(i, carry):
        f, c = i // CORNERS, i % CORNERS
        n = cn[c, f]
        col = tl[z, n]
        s = (lax.shift_right_logical(col, 3) - z + nz) & (nz - 1)
        hops = jnp.minimum(s, nz - s)
        jj = jnp.where(hops > last, rank[n], col & 7)
        off_d[i] = (s * 8 + jj) * 2
        jj = jnp.where(hops > NEAR, rank[n], col & 7)
        off_l[i] = s * 4 + lax.shift_right_logical(jj, 1) + ((jj + c) & 1) * (nz * 4)
        wgt[i] = wt[cwi[c, f]] * scale
        return carry

    lax.fori_loop(0, 128, place, 0)

    into = lanes((128, 1024))
    row = lax.broadcasted_iota(jnp.int32, (128, 1024), 0)
    local = into % 512
    wanted = (local // 64) * 16 + jnp.where(into < 512, (local % 64) // 8, 8 + local % 8)
    spread[...] = jnp.where(row == wanted, 1.0, 0.0).astype(BF16)

    def wave_step(d):
        for jj in range(NC):
            for way in range(2):
                wave(way, d, jj).wait_recv()
                wave(way, d + 1, jj).start()
            if (jj + 1) * piece % 4 == 0:
                for way in range(2):
                    correlate(slot(way, d), (jj + 1) * piece // 4 - 1)

    hear_word(0)
    hear_word(4)
    pass_word(1)
    pass_word(5)
    wave_step(1)

    wide = lanes((8, PAIRS))
    low = lax.broadcasted_iota(jnp.int32, (8, PAIRS), 0)
    to_w = jnp.where(wide // 8 == low, 1.0, 0.0)
    to_y = jnp.where(wide % 8 == low, 1.0, 0.0)
    exact = lax.Precision.HIGHEST
    row_v = jnp.dot(rv[...], to_w, precision=exact, preferred_element_type=F32)
    row_c = jnp.dot(rc[...], to_y, precision=exact, preferred_element_type=F32)
    upper.wait_recv()
    rotated = jnp.zeros((PAIRS, stack.shape[2]), F32)
    for c in range(CORNERS):
        w = wt[rwi[0, c]]
        cond = row_c[c * 8 : c * 8 + 8]
        mat = jnp.concatenate(
            [row_v[c * 8 + v : c * 8 + v + 1] * cond for v in range(8)], axis=0
        )
        mat = (w * mat * (1.0 / math.sqrt(PAIRS))).astype(BF16)
        rotated += jnp.dot(mat, stack[rn[0, c]], preferred_element_type=F32)
    rotated = rotated.astype(BF16)
    for q in range(4):
        left[q] = rotated[:, q * 128 : (q + 1) * 128]
    swap(0, 4)

    def tile_step(k):
        for way in range(2):
            tile(way, k - 1).wait_recv()
        for way in range(2):
            tile(way, k).start()
        for way in range(2):
            swap(slot(way, k - 1) * 4, 4)

    served = []
    for way in range(2):
        served += [(away(way, n), away(1 - way, last)) for n in (1, 2)]
        served += [(away(way, n), away(1 - way, NEAR)) for n in range(1, half - NEAR + 1)]
    per_way = len(served) // 2

    def starts(n, counts):
        return tuple(
            count + jnp.where(lax.shift_right_logical(tl[o, n], 3) < h, 1, 0)
            for count, (o, h) in zip(counts, served)
        )

    counts = lax.fori_loop(0, tl.shape[1], starts, (jnp.int32(0),) * len(served))
    for i, count in enumerate(counts):
        first[i] = count

    def entry(i, k):
        return tl[served[i][0], jnp.minimum(first[i] + k, tl.shape[1] - 1)] & 7

    for way in range(2):
        tile(way, 1).start()

    def both(d, carry):
        wave_step(d)
        tile_step(d)
        return carry

    hear_word(1)
    hear_word(5)
    pass_word(2)
    lax.fori_loop(2, NEAR, both, 0)
    hear_word(2)
    pass_word(3)
    wave_step(NEAR)
    tile_step(NEAR)
    hear_word(3)
    for way in range(2):
        for jj in range(NC):
            wave(way, last, jj).wait_recv()
    near = lanes((64, 128)) < 64
    for way in range(2):
        for n, (owner, k) in enumerate(
            [(0, k) for k in range(SLOTS)] + [(1, way * 2), (1, way * 2 + 1)]
        ):
            picked_w[way, n] = far_w[way, entry(way * per_way + owner, k)]
    for way in range(2):
        chosen_wave(way, True).start()
    for way in range(2):
        chosen_wave(way, False).start()
    for way in range(2):
        for j in range(2):
            correlate(slot(way, last), j, way)

    for way in range(2):
        tile(way, NEAR).wait_recv()
    for way in range(2):
        s = slot(way, NEAR)
        for q in range(4):
            v = near_t[way, q]
            turned = pltpu.roll(v.astype(F32), 64, 1).astype(BF16)
            near_t[way, 4 + q] = turned
            left[s * 4 + q] = v
            left[nz * 4 + s * 4 + q] = turned
        for n in range(half - NEAR):
            for q in range(2):
                lo = entry(way * per_way + 2 + n, 2 * q)
                hi = entry(way * per_way + 2 + n, 2 * q + 1)
                a = near_t[way, lax.shift_right_logical(lo, 1) + (lo & 1) * 4]
                b = near_t[way, lax.shift_right_logical(hi, 1) + ((hi + 1) & 1) * 4]
                picked_t[way, n, q] = jnp.where(near, a, b)
    for way in range(2):
        chosen_wave(way, True).wait_recv()
        last_wave(way).start()
    for way in range(2):
        chosen_wave(way, False).wait_recv()
        correlate(slot(way, half - 1), 0)
    for way in range(2):
        last_wave(way).wait_recv()
    correlate(half, 0)

    for k in range(half, NEAR, -1):
        for way in range(2):
            far_tile(way, k).start()

    lane = lanes((8, 128))

    def pick(i, side):
        c = side * nx + i
        for t in range(2):
            acc = jnp.zeros((8, 128), F32)
            for ff in range(8):
                n = (t * 8 + ff) * CORNERS + c
                val = dense[off_d[n], :, t * 128 : t * 128 + 128] * wgt[n]
                cond = dense[off_d[n] + 1, :, t * 128 : t * 128 + 128]
                acc = jnp.where(lane // 8 == 2 * ff, val, acc)
                acc = jnp.where(lane // 8 == 2 * ff + 1, cond, acc)
            sel[c, :, pl.ds(t * 128, 128)] = acc
        return side

    lax.fori_loop(0, nx, pick, 1 - core)

    to_core = pltpu.make_async_remote_copy(
        src_ref=sel.at[pl.ds((1 - core) * nx, nx)],
        dst_ref=from_core,
        send_sem=core_s.at[0],
        recv_sem=core_r.at[0],
        device_id=(partner, z),
        device_id_type=MESH,
    )

    def to_x(r):
        return pltpu.make_async_remote_copy(
            src_ref=part,
            dst_ref=from_x.at[r - 1],
            send_sem=x_s.at[r - 1],
            recv_sem=x_r.at[r - 1],
            device_id=(x_peer(r), z),
            device_id_type=MESH,
        )

    def to_y(r):
        return pltpu.make_async_remote_copy(
            src_ref=sum1,
            dst_ref=from_y.at[r - 1],
            send_sem=y_s.at[r - 1],
            recv_sem=y_r.at[r - 1],
            device_id=(y_peer(r), z),
            device_id_type=MESH,
        )

    def across(arriving=False):
        mine = 1 - core if arriving else core
        return pltpu.make_async_remote_copy(
            src_ref=full.at[pl.ds(core * nx, nx)],
            dst_ref=full.at[pl.ds(mine * nx, nx)],
            send_sem=core_s.at[1],
            recv_sem=core_r.at[1],
            device_id=(partner, z),
            device_id_type=MESH,
        )

    to_core.start()
    lax.fori_loop(0, nx, pick, core)
    to_core.wait_recv()
    total = sel[pl.ds(core * nx, nx)] + from_core[...]
    part[...] = total
    for r in range(1, nx):
        to_x(r).start()
    for r in range(1, nx):
        to_x(r).wait_recv()
        total += from_x[r - 1]
    sum1[...] = total
    for r in range(1, ny):
        to_y(r).start()
    upper.wait_send()

    def sent(d, carry):
        for way in range(2):
            for j in range(NC):
                wave(way, d, j).wait_send()

            @pl.when(d <= NEAR)
            def _():
                tile(way, d).wait_send()

        return carry

    lax.fori_loop(1, last + 1, sent, 0)
    for way in range(2):
        chosen_wave(way, True).wait_send()
        chosen_wave(way, False).wait_send()
        last_wave(way).wait_send()
        for k in range(NEAR + 1, half + 1):
            far_tile(way, k).wait_send()

    for r in range(1, ny):
        to_y(r).wait_recv()
        total += from_y[r - 1]
    full[pl.ds(core * nx, nx)] = total
    across().start()
    for k in range(NEAR + 1, half):
        for way in range(2):
            far_tile(way, k).wait_recv()
            swap(slot(way, k) * 4, 2)
    for way in range(2):
        far_tile(way, half).wait_recv()
    swap(half * 4, 2)
    def rotations(side):
        rows = nx * 8
        corr = full[pl.ds(side * nx, nx)].reshape(rows, 256)
        corr = jnp.concatenate([corr[:, :128], corr[:, 128:]], axis=0)
        high = corr.astype(BF16)
        rest = (corr - high.astype(F32)).astype(BF16)
        expanded[...] = jnp.dot(high, spread[...], preferred_element_type=F32) + jnp.dot(
            rest, spread[...], preferred_element_type=F32
        )

        def rotate(c, carry):
            for t in range(2):
                at = pl.multiple_of(t * rows + c * 8, 8)
                val = expanded[pl.ds(at, 8), pl.ds(0, 512)]
                cond = expanded[pl.ds(at, 8), pl.ds(512, 512)]
                for w in range(0, 8, 2):
                    both_w = jnp.concatenate(
                        [val[w : w + 1] * cond, val[w + 1 : w + 2] * cond], 0
                    )
                    to = pl.multiple_of((side * nx + c) * 64 + w * 8, 16)
                    rsm[pl.ds(to, 16), pl.ds(t * 512, 512)] = both_w.astype(BF16)
            return carry

        lax.fori_loop(0, nx, rotate, 0)

    def products(side, add):
        for p in range(8):
            blocks = []
            for ff in range(2):
                at = (p * 2 + ff) * CORNERS + side * nx
                quads = []
                for q in range(2):
                    a, b = left[off_l[at + 2 * q]], left[off_l[at + 2 * q + 1]]
                    quads.append(jnp.where(near, a, b))
                blocks.append(jnp.concatenate(quads, axis=1))
            res = jnp.dot(
                jnp.concatenate(blocks, axis=0),
                rsm[pl.ds(side * 256, 256), p * 128 : (p + 1) * 128],
                preferred_element_type=F32,
            )
            if add:
                res += mixed[p * 128 : (p + 1) * 128]
                turned = pltpu.roll(res, 64, 1)
                even = jnp.where(near, res[:64], turned[:64])
                odd = jnp.where(near, turned[64:], res[64:])
                res = jnp.concatenate([even, odd], axis=0)
            mixed[p * 128 : (p + 1) * 128] = res

    rotations(core)
    products(core, False)
    across(True).wait_recv()
    rotations(1 - core)
    products(1 - core, True)

    near_f = lanes((16, 128)) < 64
    def put(i):
        part_of = pl.ds(i * 1024, 1024)
        return pltpu.make_async_copy(out.at[:, part_of], out_hbm.at[:, part_of], in_sem.at[i])

    for t in range(32):
        even = mixed[pl.ds(2 * t, 16, stride=64), :]
        odd = mixed[pl.ds(2 * t + 1, 16, stride=64), :]
        out[:, t * 128 : (t + 1) * 128] = jnp.where(near_f, even, odd).astype(BF16)
        if t % 8 == 7:
            put(t // 8).start()
    to_core.wait_send()
    for r in range(1, nx):
        to_x(r).wait_send()
    for r in range(1, ny):
        to_y(r).wait_send()
    across().wait_send()
    for i in range(4):
        put(i).wait()


def body(mesh_shape, *args):
    (fine_waves, coarse_waves, coarse_kernel, row_valence, row_conduction, row_neighbours,
     row_weight_index, col_neighbours, col_weight_index, tile_list, weight_table) = args
    nz, ng = mesh_shape
    nx = CORNERS // 2
    ny = ng // CORNERS
    width = fine_waves.shape[2]
    held = coarse_waves.shape[0]
    any_space = pl.BlockSpec(memory_space=pl.ANY)
    smem = pltpu.SMEM
    half = nz // 2
    dma = pltpu.SemaphoreType.DMA
    out = pl.pallas_call(
        functools.partial(kernel, nz, nx, ny),
        out_shape=jax.ShapeDtypeStruct((16, PAIRS * PAIRS), BF16),
        in_specs=[any_space] * 11,
        out_specs=any_space,
        scratch_shapes=[
            pltpu.VMEM((16, PAIRS * PAIRS), BF16),
            pltpu.VMEM((64, 8), F32),
            pltpu.VMEM((64, 8), F32),
            smem((1, CORNERS), jnp.int32),
            smem((1, CORNERS), jnp.int32),
            smem((CORNERS, 16), jnp.int32),
            smem((CORNERS, 16), jnp.int32),
            smem(tile_list.shape, jnp.int32),
            smem(weight_table.shape, F32),
            pltpu.VMEM((256, width), BF16),
            pltpu.VMEM((nz, held, BANDS, width), BF16),
            pltpu.VMEM((2, held, BANDS, width), BF16),
            pltpu.VMEM((nz * held * 2, 8, 256), F32),
            pltpu.VMEM((12, PAIRS, 512), BF16),
            pltpu.VMEM((2 * nz * 4, PAIRS, 128), BF16),
            pltpu.VMEM((2, 8, PAIRS, 128), BF16),
            pltpu.VMEM((128, 1024), BF16),
            pltpu.VMEM((64, 1024), F32),
            pltpu.VMEM((512, 1024), BF16),
            pltpu.VMEM((1024, 128), F32),
            pltpu.VMEM((2, SLOTS * 3 // 2, BANDS, width), BF16),
            pltpu.VMEM((2, half - NEAR, 2, PAIRS, 128), BF16),
            pltpu.VMEM((CORNERS, 8, 256), F32),
            pltpu.VMEM((nx, 8, 256), F32),
            pltpu.VMEM((nx, 8, 256), F32),
            pltpu.VMEM((nx - 1, nx, 8, 256), F32),
            pltpu.VMEM((nx, 8, 256), F32),
            pltpu.VMEM((ny - 1, nx, 8, 256), F32),
            pltpu.VMEM((CORNERS, 8, 256), F32),
            pltpu.SMEM((128,), jnp.int32),
            pltpu.SMEM((128,), jnp.int32),
            pltpu.SMEM((128,), F32),
            pltpu.SMEM((32,), jnp.int32),
            pltpu.SMEM((32,), jnp.int32),
            dma((11,)),
            dma((2, half, NC)),
            dma((2, half, NC)),
            dma,
            dma,
            dma((2, NEAR)),
            dma((2, NEAR)),
            dma((2, half - NEAR)),
            dma((2, half - NEAR)),
            dma((2,)),
            dma((2,)),
            dma((nx - 1,)),
            dma((nx - 1,)),
            dma((ny - 1,)),
            dma((ny - 1,)),
            pltpu.SemaphoreType.REGULAR((6,)),
        ],
        compiler_params=pltpu.CompilerParams(
            collective_id=0, has_side_effects=True, vmem_limit_bytes=60 * 1024 * 1024
        ),
        name="interpolate",
    )(
        fine_waves.reshape(16 * BANDS, width),
        coarse_waves,
        coarse_kernel,
        row_valence.reshape(64, 8),
        row_conduction.reshape(64, 8),
        row_neighbours,
        row_weight_index,
        col_neighbours.T,
        col_weight_index.T,
        tile_list,
        weight_table,
    )
    return out[None]


def solution(mesh):
    placed = (
        P("ka", None, "ga"),
        P("ka", None, "ga"),
        P("ga", None, "ka"),
        P("ga", None, None, None),
        P("ga", None, None, None),
        P("ga", None),
        P("ga", None),
        P("ka", None),
        P("ka", None),
        P(),
        P(),
    )
    shape = (mesh.shape["ka"], mesh.shape["ga"])
    return jax.shard_map(
        functools.partial(body, shape),
        mesh=mesh,
        in_specs=placed,
        out_specs=P("ga", "ka", None),
        check_vma=False,
    )
```
